256 devices in a mesh: rows: 128 (over y, x, z_lo, core), cols: 2 (over z_hi).
Axes of the slice: x: 4, y: 4, z: 8 (z_hi: 2, z_lo: 4; z = z_hi * 4 + z_lo), core: 2. Of those that a mesh axis runs over, the one named last changes fastest.
Arguments:
- eigvecs: float32 [32768, 2048], P('rows', 'cols'), may hold values from -6 to 6
- reflectors: float32 [32, 32768], P('cols', 'rows'), may hold values from -17 to 17
- starts: int32 [32], replicated, may hold values from 0 to 63
Outputs:
- rotated: float32 [32768, 2048], P('rows', 'cols')
The draws below stay inside these ranges and needn't reach their ends.
Inputs may be any that keep to these rules, and one draw needn't show every extreme that they name: Sweep j's windows begin at rows starts[j] + k * 64.
All inputs are finite; a program needn't handle non-finite values.
Results may differ from the reference program's by a relative error of at most 0.00011.
Values sent between devices are 32-bit elements; how exact they have to be, the bound alone decides.
No kernel may reach another device: no remote copies, remote signals or barrier semaphores. Data moves between devices by JAX's collectives and lax.ppermute only.
A program may use at most 64 MiB of HBM per device.

```python
import math
import jax
import jax.numpy as jnp
from jax import lax

BAND = 64
COLS = 2048
SWEEPS = 32
ORDER = 32768


def draw_reflectors(key, part):
    scale_key = jax.random.fold_in(key, 11)
    value_key = jax.random.fold_in(key, 12)
    extent = (SWEEPS, ORDER)
    scales = jnp.exp(jax.random.uniform(scale_key, extent, jnp.float32, math.log(0.3), math.log(3.0)))
    random_part = jnp.clip(jax.random.normal(value_key, extent, jnp.float32), -4.0, 4.0)
    return (random_part * scales).astype(jnp.float32)


def place_ends(values, key, low, high):
    longest = values.shape.index(max(values.shape))
    spots = []
    for shift in (0, 1):
        where = [jax.random.randint(jax.random.fold_in(key, axis), (), 0, length) for axis, length in enumerate(values.shape)]
        where[longest] = (where[longest] + shift) % values.shape[longest]
        spots.append(tuple(where))
    return values.at[spots[0]].set(low).at[spots[1]].set(high)


def levels(key, shape, cuts, smallest, high):
    loudness, own = 1.0, jax.random.fold_in(key, 6)
    for dim, parts in cuts:
        draws = jnp.exp(jax.random.uniform(jax.random.fold_in(own, dim), (parts,), jnp.float32, smallest / len(cuts), high / len(cuts)))
        loudness = loudness * jnp.repeat(draws, shape[dim] // parts).reshape([-1 if axis == dim else 1 for axis in range(len(shape))])
    return loudness


def centred(stream_key, dims, scale, limit, pieces=(), kind=jnp.bfloat16):
    result = scale * jax.random.normal(stream_key, dims, jnp.float32)
    if pieces:
        result = result * levels(stream_key, dims, pieces, -0.22, 0.18)
    return jnp.clip(result, -limit, limit).astype(kind)


def setup_inputs(seed: int = 0) -> dict:
    keys = jax.random.split(jax.random.key(seed), 4)
    eigvecs = centred(keys[0], (ORDER, COLS), 1.0, 6.0, ((0, 128), (1, 2)), jnp.float32)
    reflectors = draw_reflectors(jax.random.fold_in(keys[3], 71), 0)
    starts = place_ends(jax.random.randint(keys[2], (SWEEPS,), 0, BAND), jax.random.fold_in(keys[2], 1), 0, BAND - 1).astype(jnp.int32)
    return {"eigvecs": eigvecs, "reflectors": reflectors, "starts": starts}


def one_sweep(vectors, reflector, offset):
    total_rows = vectors.shape[0]
    blocks = total_rows // BAND
    rolled = jnp.roll(vectors, -offset, axis=0).reshape(blocks, BAND, vectors.shape[1])
    rolled_v = jnp.roll(reflector, -offset).reshape(blocks, BAND)
    squares = jnp.sum(rolled_v * rolled_v, axis=1)
    window = jnp.arange(blocks, dtype=jnp.int32)
    usable = (window + 1) * BAND + offset <= total_rows
    scaled = jnp.where(usable, 2.0 / jnp.where(usable, squares, 1.0), 0.0)
    products = jnp.einsum("kb,kbm->km", rolled_v, rolled, precision=lax.Precision.HIGHEST)
    rolled = rolled - rolled_v[:, :, None] * (scaled[:, None] * products)[:, None, :]
    return jnp.roll(rolled.reshape(total_rows, vectors.shape[1]), offset, axis=0)


def reference(eigvecs, reflectors, starts):
    def advance(sweep_idx, vectors):
        return one_sweep(vectors, reflectors[sweep_idx], starts[sweep_idx])
    return lax.fori_loop(0, SWEEPS, advance, eigvecs)
```

```python
import jax
import jax.numpy as jnp
from jax import lax
from jax.experimental import pallas as pl
from jax.experimental.pallas import tpu as pltpu
from jax.sharding import PartitionSpec as P

BAND = 64
SWEEPS = 32
LANES = 128
HALF = SWEEPS // 2
QUARTER = SWEEPS // 4


def dot(a, b, contract=((1,), (0,))):
    return lax.dot_general(
        a, b, (contract, ((), ())), precision=lax.Precision.HIGHEST, preferred_element_type=jnp.float32
    )


def lane_of(shape):
    return lax.broadcasted_iota(jnp.int32, shape, len(shape) - 1)


def row_of(shape):
    return lax.broadcasted_iota(jnp.int32, shape, 0)


def call(kernel, outs, *args, flops=1_000_000):
    nbytes = 4 * sum(a.size for a in args)
    return pl.pallas_call(
        kernel,
        out_shape=[jax.ShapeDtypeStruct(s, jnp.float32) for s in outs],
        in_specs=[pl.BlockSpec(memory_space=pltpu.VMEM)] * len(args),
        out_specs=[pl.BlockSpec(memory_space=pltpu.VMEM)] * len(outs),
        compiler_params=pltpu.CompilerParams(vmem_limit_bytes=16 * 1024 * 1024),
        cost_estimate=pl.CostEstimate(flops=flops, bytes_accessed=nbytes, transcendentals=0),
    )(*args)


def place():
    index = lax.axis_index("rows")
    return index % 2, (index // 2) % 2, index // 2


def factor_kernel(own_ref, other_ref, start_ref, x_ref, a_ref, msg_ref, coef_ref, inner_ref, proj_ref, edge_ref):
    first = lax.axis_index("cols") == 0
    own, other = own_ref[...], other_ref[...]
    r = jnp.concatenate([jnp.where(first, own, other), jnp.where(first, other, own)], axis=0)
    rows = r.shape[1]
    start = start_ref[:, 0:1]
    segment = (lane_of(r.shape) - start + BAND) >> 6
    parts = [jnp.where(segment == k, r, 0.0) for k in range(5)]
    zero = jnp.zeros_like(r)
    inner = jnp.concatenate(parts[1:4], axis=0)
    edge = jnp.concatenate([parts[0], parts[4]], axis=0)
    left = jnp.concatenate([inner, zero, edge], axis=0)
    right = jnp.concatenate([inner, zero, edge, zero, zero], axis=0)
    gram = dot(left, right, ((1,), (1,)))
    earlier = (lane_of(gram.shape) & (SWEEPS - 1)) < (row_of(gram.shape) & (SWEEPS - 1))
    gram = jnp.where(earlier, gram, 0.0)
    count = 3 * SWEEPS
    tau = 2.0 / jnp.sum(inner * inner, axis=1, keepdims=True)
    lower = tau * gram[0:count, 0:LANES]
    rhs = tau * jnp.concatenate([inner, gram[0:count, LANES : 2 * LANES]], axis=1)
    blocks = [[rhs[32 * k + 8 * q : 32 * k + 8 * q + 8] for q in range(4)] for k in range(3)]
    for j in range(SWEEPS - 1):
        source = [blocks[k][j // 8][j % 8 : j % 8 + 1] for k in range(3)]
        for k in range(3):
            for q in range((j + 1) // 8, 4):
                at = 32 * k + 8 * q
                total = blocks[k][q]
                for m in range(3):
                    if abs(m - k) < 2:
                        column = 32 * m + j
                        total = total - lower[at : at + 8, column : column + 1] * source[m]
                blocks[k][q] = total
    solved = jnp.concatenate([blocks[k][q] for k in range(3) for q in range(4)] + [jnp.zeros((32, rhs.shape[1]), jnp.float32)], axis=0)
    back = dot(gram[LANES : LANES + 64, 0:LANES], solved)
    observe = edge - back[:, 0:rows]
    couple = back[:, rows:] - gram[LANES : LANES + 64, LANES : 2 * LANES]
    squares = jnp.sum(edge * edge, axis=1, keepdims=True)
    coef = jnp.where(lane_of(couple.shape) == 64, squares, couple)
    coef_ref[...] = coef
    inner_ref[...] = inner
    proj_ref[...] = solved[0:count, 0:rows]
    edge_ref[...] = edge - dot(solved[0:count, rows : rows + 64], inner, ((0,), (0,)))
    a = dot(observe, x_ref[...])
    half = a.shape[1] // 2
    core, _, _ = place()
    low, high = a[:, 0:half], a[:, half:]
    a_ref[...] = jnp.where(core == 0, low, high)
    msg_ref[...] = jnp.concatenate([jnp.where(core == 0, high, low), coef], axis=1)


def merge_kernel(a_ref, coef_ref, msg_ref, mid_ref, even_ref, odd_ref, out_ref):
    core, parity, _ = place()
    half = a_ref.shape[1]
    mine = jnp.concatenate([a_ref[...], coef_ref[...]], axis=1)
    theirs = msg_ref[...]
    top = jnp.where(core == 0, mine, theirs)
    low = jnp.where(core == 0, theirs, mine)
    tc, lc = top[:, half:], low[:, half:]
    tau = 2.0 / (tc[32:64, 64:65] + lc[0:32, 64:65])
    lane = lane_of(tc.shape)
    tk = jnp.where(lane < 32, tc, 0.0)
    lk = jnp.where((lane >= 32) & (lane < 64), lc, 0.0)
    mid = jnp.concatenate([top[32:64, 0:half] + low[0:32, 0:half], tk[32:64] + lk[0:32]], axis=1) * tau
    left = jnp.concatenate([top[0:32, 0:half], tk[0:32]], axis=1)
    right = jnp.concatenate([low[32:64, 0:half], lk[32:64]], axis=1)
    into_left, into_right = tc[0:32], lc[32:64]
    own_top, own_low = tc[32:64] * tau, lc[0:32] * tau
    blocks = [mid[8 * q : 8 * q + 8] for q in range(4)]
    for j in range(SWEEPS):
        source = blocks[j // 8][j % 8 : j % 8 + 1]
        for q in range((j + 1) // 8, 4):
            at = 8 * q
            weight = own_top[at : at + 8, 32 + j : 33 + j] + own_low[at : at + 8, j : j + 1]
            blocks[q] = blocks[q] + weight * source
        left = left + into_left[:, 32 + j : 33 + j] * source
        right = right + into_right[:, j : j + 1] * source
    mid = jnp.concatenate(blocks, axis=0)

    def ordered(block):
        tile = block[:, half:]
        at = lane_of(tile.shape)
        swapped = jnp.where(at < 32, pltpu.roll(tile, 96, 1), pltpu.roll(tile, 32, 1))
        return jnp.where(at < 64, jnp.where(parity == 0, swapped, tile), 0.0)

    spot = lane_of((32, LANES)) == 64
    left_tile = jnp.where(spot, tc[0:32, 64:65], ordered(left))
    right_tile = jnp.where(spot, lc[32:64, 64:65], ordered(right))
    even_a = jnp.where(parity == 0, right[:, 0:half], left[:, 0:half])
    odd_a = jnp.where(parity == 0, left[:, 0:half], right[:, 0:half])
    even_t = jnp.where(parity == 0, right_tile, left_tile)
    odd_t = jnp.where(parity == 0, left_tile, right_tile)
    mid_ref[...] = jnp.concatenate([mid[:, 0:half], ordered(mid)], axis=1)
    even_ref[...] = jnp.concatenate([even_a, even_t], axis=1)
    odd_ref[...] = jnp.concatenate([odd_a, odd_t], axis=1)
    out_ref[...] = jnp.concatenate([even_a[0:8]] + [even_t[8 * q : 8 * q + 8] for q in range(4)], axis=1)


def substitute(block, lower, first, lane):
    for j in range(block.shape[0] - 1):
        block = block + lower[first : first + block.shape[0], lane + first + j : lane + first + j + 1] * block[j : j + 1]
    return block


def spread(rows, tile, at, solved, lane):
    for j in range(solved.shape[0]):
        rows = rows + tile[at : at + rows.shape[0], lane + j : lane + j + 1] * solved[j : j + 1]
    return rows


def even0_kernel(msg_ref, even_ref, odd_ref, w_ref, pair_ref, even_out, odd_out, out_ref):
    half = even_ref.shape[1] - LANES
    got = msg_ref[...]
    tile = even_ref[:, half:]
    other = jnp.concatenate([got[:, half + LANES * q : half + LANES * (q + 1)] for q in range(4)], axis=0)
    both = tile + other
    tau = 2.0 / both[:, 64:65]
    lower = tau * both
    pair_ref[...] = jnp.where(lane_of(lower.shape) == 64, tau, lower)
    w = substitute((even_ref[0:8, 0:half] + got[:, 0:half]) * tau[0:8], lower, 0, 0)
    w_ref[...] = w
    odd_tile = odd_ref[:, half:]
    odd = spread(odd_ref[:, 0:half], odd_tile, 0, w, 0)
    out_ref[...] = jnp.concatenate([odd[0:16], odd_tile[0:16], odd_tile[16:32]], axis=1)
    odd_out[...] = odd
    even_out[...] = spread(even_ref[8:32, 0:half], tile, 8, w, 0)


def odd0_kernel(msg_ref, start_ref, even_ref, odd_ref, even_t_ref, odd_t_ref, w_ref, pair_ref, even_out, odd_out, out_ref):
    half = even_ref.shape[1]
    _, _, chip = place()
    got = msg_ref[...]
    tile = odd_t_ref[...]
    both = tile + jnp.concatenate([got[:, half : half + LANES], got[:, half + LANES :]], axis=0)
    chips = lax.axis_size("rows") // 2
    valid = (chip > 0) & ((chip < chips - 1) | (start_ref[:, 0:1] == 0))
    tau = jnp.where(valid, 2.0 / jnp.where(valid, both[:, 64:65], 1.0), 0.0)
    lower = tau * both
    pair_ref[...] = jnp.where(lane_of(lower.shape) == 64, tau, lower)
    w = substitute((odd_ref[0:16] + got[:, 0:half]) * tau[0:16], lower, 0, 32)
    w_ref[...] = w
    even = spread(even_ref[...], even_t_ref[...], 8, w, 32)
    out_ref[...] = even[0:16]
    even_out[...] = even
    odd_out[...] = spread(odd_ref[16:32], tile, 16, w, 32)


def even1_kernel(msg_ref, pair_ref, even_ref, odd_ref, even_t_ref, odd_t_ref, w_ref, even_out, out_ref):
    pair = pair_ref[...]
    w = substitute((even_ref[0:16] + msg_ref[...]) * pair[8:24, 64:65], pair, 8, 0)
    w_ref[...] = w
    out_ref[...] = spread(odd_ref[...], odd_t_ref[...], 16, w, 8)
    even_out[...] = spread(even_ref[16:24], even_t_ref[...], 24, w, 8)


def odd1_kernel(msg_ref, pair_ref, odd_ref, even_ref, even_t_ref, w_ref, out_ref):
    pair = pair_ref[...]
    w = substitute((odd_ref[...] + msg_ref[...]) * pair[16:32, 64:65], pair, 16, 32)
    w_ref[...] = w
    out_ref[...] = spread(even_ref[...], even_t_ref[...], 24, w, 48)


def even2_kernel(msg_ref, pair_ref, even_ref, mid_ref, e0_ref, e1_ref, o0_ref, o1_ref, keep_ref, out_ref):
    core, parity, _ = place()
    half = even_ref.shape[1]
    pair = pair_ref[...]
    w = substitute((even_ref[...] + msg_ref[...]) * pair[24:32, 64:65], pair, 24, 0)
    even = jnp.concatenate([e0_ref[...], e1_ref[...], w], axis=0)
    odd = jnp.concatenate([o0_ref[...], o1_ref[...]], axis=0)
    mid = mid_ref[:, 0:half]
    tile = mid_ref[:, half:]
    mid = spread(spread(mid, tile, 0, even, 0), tile, 0, odd, 32)
    left = jnp.where(parity == 0, odd, even)
    right = jnp.where(parity == 0, even, odd)
    upper = jnp.concatenate([left, mid], axis=0)
    lower = jnp.concatenate([mid, right], axis=0)
    keep_ref[...] = jnp.where(core == 0, upper, lower)
    out_ref[...] = jnp.where(core == 0, lower, upper)


def inner_kernel(inner_ref, proj_ref, x_ref, y_ref):
    x = x_ref[...]
    y_ref[...] = x - dot(inner_ref[...], dot(proj_ref[...], x), ((0,), (0,)))


def final_kernel(edge_ref, keep_ref, msg_ref, y_ref, out_ref):
    core, _, _ = place()
    keep, got = keep_ref[...], msg_ref[...]
    w = jnp.concatenate([jnp.where(core == 0, keep, got), jnp.where(core == 0, got, keep)], axis=1)
    out_ref[...] = y_ref[...] - dot(edge_ref[...], w, ((0,), (0,)))


def per_device(eigvecs, reflectors, starts):
    count = lax.axis_size("rows")
    rows, cols = eigvecs.shape
    half = cols // 2
    wide = half + LANES
    on_chip = [(i, i ^ 1) for i in range(count)]
    even_pairs = [(i, i ^ 2) for i in range(count)]
    odd_pairs = [(i, ((i - 2) ^ 2) + 2) for i in range(2, count - 2)]
    start = jnp.broadcast_to(starts[:, None], (SWEEPS, LANES))
    other = lax.ppermute(reflectors, "cols", [(0, 1), (1, 0)])
    a, msg, coef, inner, proj, edge = call(
        factor_kernel,
        [(64, half), (64, wide), (64, LANES), (96, rows), (96, rows), (64, rows)],
        reflectors, other, start, eigvecs,
    )
    got = lax.ppermute(msg, "rows", on_chip)
    mid, even, odd, msg = call(merge_kernel, [(32, wide), (32, wide), (32, wide), (8, half + 4 * LANES)], a, coef, got)
    even_t, odd_t = even[:, half:], odd[:, half:]
    got = lax.ppermute(msg, "rows", even_pairs)
    (partial,) = call(inner_kernel, [(rows, cols)], inner, proj, eigvecs, flops=20_000_000)
    e0, even_pair, even, odd, msg = call(
        even0_kernel, [(8, half), (32, LANES), (24, half), (32, half), (16, half + 2 * LANES)], got, even, odd
    )
    got = lax.ppermute(msg, "rows", odd_pairs)
    o0, odd_pair, even, odd, msg = call(
        odd0_kernel, [(16, half), (32, LANES), (24, half), (16, half), (16, half)], got, start, even, odd, even_t, odd_t
    )
    got = lax.ppermute(msg, "rows", even_pairs)
    e1, even, odd = call(even1_kernel, [(16, half), (8, half), (16, half)], got, even_pair, even, odd, even_t, odd_t)
    got = lax.ppermute(odd, "rows", odd_pairs)
    o1, even = call(odd1_kernel, [(16, half), (8, half)], got, odd_pair, odd, even, even_t)
    got = lax.ppermute(even, "rows", even_pairs)
    keep, msg = call(even2_kernel, [(64, half), (64, half)], got, even_pair, even, mid, e0, e1, o0, o1)
    got = lax.ppermute(msg, "rows", on_chip)
    (out,) = call(final_kernel, [(rows, cols)], edge, keep, got, partial)
    return out


def solution(mesh):
    in_specs = (P("rows", "cols"), P("cols", "rows"), P())
    out_specs = P("rows", "cols")
    return jax.shard_map(
        per_device, mesh=mesh, in_specs=in_specs, out_specs=out_specs, check_vma=False
    )
```

```python
import jax
import jax.numpy as jnp
from jax import lax
from jax.experimental import pallas as pl
from jax.experimental.pallas import tpu as pltpu
from jax.sharding import PartitionSpec as P

BAND = 64
SWEEPS = 32
LANES = 128


def dot(a, b, contract=((1,), (0,))):
    return lax.dot_general(
        a, b, (contract, ((), ())), precision=lax.Precision.HIGHEST, preferred_element_type=jnp.float32
    )


def lane_of(shape):
    return lax.broadcasted_iota(jnp.int32, shape, len(shape) - 1)


def row_of(shape):
    return lax.broadcasted_iota(jnp.int32, shape, 0)


def call(kernel, outs, *args, flops=1_000_000):
    nbytes = 4 * sum(a.size for a in args)
    return pl.pallas_call(
        kernel,
        out_shape=[jax.ShapeDtypeStruct(s, jnp.float32) if isinstance(s, tuple) else s for s in outs],
        in_specs=[pl.BlockSpec(memory_space=pltpu.VMEM)] * len(args),
        out_specs=[pl.BlockSpec(memory_space=pltpu.VMEM)] * len(outs),
        compiler_params=pltpu.CompilerParams(vmem_limit_bytes=16 * 1024 * 1024),
        cost_estimate=pl.CostEstimate(flops=flops, bytes_accessed=nbytes, transcendentals=0),
    )(*args)


def split(a):
    high = a.astype(jnp.bfloat16)
    return high, (a - high.astype(jnp.float32)).astype(jnp.bfloat16)


def dot3(a, b, contract=((1,), (0,))):
    (ah, al), (bh, bl) = split(a), b if isinstance(b, tuple) else split(b)

    def one(x, y):
        return lax.dot_general(x, y, (contract, ((), ())), preferred_element_type=jnp.float32)

    return one(ah, bh) + (one(ah, bl) + one(al, bh))


def ready_kernel(x_ref, own_ref, start_ref, high_ref, low_ref, copy_ref, column_ref):
    high_ref[...], low_ref[...] = split(x_ref[...])
    copy_ref[...] = own_ref[...]
    square = (SWEEPS, SWEEPS)
    row = start_ref[...].astype(jnp.float32)
    column = jnp.sum(jnp.where(lane_of(square) == row_of(square), row, 0.0), axis=1, keepdims=True)
    column_ref[...] = jnp.broadcast_to(column, (SWEEPS, LANES))


def factor_kernel(own_ref, other_ref, start_ref, high_ref, low_ref, msg_ref, inner_ref, proj_ref, edge_ref):
    first = lax.axis_index("cols") == 0
    own, other = own_ref[...], other_ref[...]
    r = jnp.concatenate([jnp.where(first, own, other), jnp.where(first, other, own)], axis=0)
    rows = r.shape[1]
    start = start_ref[:, 0:1].astype(jnp.int32)
    segment = (lane_of(r.shape) - start + BAND) >> 6
    parts = [jnp.where(segment == k, r, 0.0) for k in range(5)]
    zero = jnp.zeros_like(r)
    inner = jnp.concatenate(parts[1:4], axis=0)
    edge = jnp.concatenate([parts[0], parts[4]], axis=0)
    left = jnp.concatenate([inner, zero, edge], axis=0)
    right = jnp.concatenate([inner, zero, edge, zero, zero], axis=0)
    gram = dot(left, right, ((1,), (1,)))
    earlier = (lane_of(gram.shape) & (SWEEPS - 1)) < (row_of(gram.shape) & (SWEEPS - 1))
    gram = jnp.where(earlier, gram, 0.0)
    count = 3 * SWEEPS
    tau = 2.0 / jnp.sum(inner * inner, axis=1, keepdims=True)
    lower = tau * gram[0:count, 0:LANES]
    rhs = tau * jnp.concatenate([inner, gram[0:count, LANES : 2 * LANES]], axis=1)
    blocks = [[rhs[32 * k + 8 * q : 32 * k + 8 * q + 8] for q in range(4)] for k in range(3)]
    for j in range(SWEEPS - 1):
        source = [blocks[k][j // 8][j % 8 : j % 8 + 1] for k in range(3)]
        for k in range(3):
            for q in range((j + 1) // 8, 4):
                at = 32 * k + 8 * q
                total = blocks[k][q]
                for m in range(3):
                    if abs(m - k) < 2:
                        column = 32 * m + j
                        total = total - lower[at : at + 8, column : column + 1] * source[m]
                blocks[k][q] = total
    solved = jnp.concatenate([blocks[k][q] for k in range(3) for q in range(4)] + [jnp.zeros((32, rhs.shape[1]), jnp.float32)], axis=0)
    back = dot(gram[LANES : LANES + 64, 0:LANES], solved)
    observe = edge - back[:, 0:rows]
    couple = back[:, rows:] - gram[LANES : LANES + 64, LANES : 2 * LANES]
    squares = jnp.sum(edge * edge, axis=1, keepdims=True)
    coef = jnp.where(lane_of(couple.shape) == 64, squares, couple)
    inner_ref[...] = inner
    proj_ref[...] = solved[0:count, 0:rows]
    edge_ref[...] = edge - dot(solved[0:count, rows : rows + 64], inner, ((0,), (0,)))
    msg_ref[...] = jnp.concatenate([dot3(observe, (high_ref[...], low_ref[...])), coef], axis=1)


def to_low(tile):
    return jnp.where(lane_of(tile.shape) < 32, pltpu.roll(tile, LANES - 32, 1), 0.0)


def solve(blocks, lower, lane=0):
    for j in range(SWEEPS):
        source = blocks[j // 8][j % 8 : j % 8 + 1]
        for q in range((j + 1) // 8, len(blocks)):
            blocks[q] = blocks[q] + lower[8 * q : 8 * q + 8, lane + j : lane + j + 1] * source
    return jnp.concatenate(blocks, axis=0)


def spread(rows, tile, at, solved, lane):
    for j in range(solved.shape[0]):
        rows = rows + tile[at : at + rows.shape[0], lane + j : lane + j + 1] * solved[j : j + 1]
    return rows


def substitute(block, lower, first, lane):
    for j in range(block.shape[0] - 1):
        block = block + lower[first : first + block.shape[0], lane + first + j : lane + first + j + 1] * block[j : j + 1]
    return block


def chip_of():
    return lax.axis_index("rows") // 2


def merge_kernel(own_ref, got_ref, mid_ref, e_ref, o_ref):
    even = chip_of() % 2 == 0
    cols = own_ref.shape[1] - LANES
    top, low = got_ref[...], own_ref[...]
    tc, lc = top[:, cols:], low[:, cols:]
    tau = 2.0 / (tc[32:64, 64:65] + lc[0:32, 64:65])
    lane = lane_of(tc.shape)
    tk = jnp.where(lane < 32, tc, 0.0)
    lk = jnp.where((lane >= 32) & (lane < 64), lc, 0.0)
    mid = jnp.concatenate([top[32:64, 0:cols] + low[0:32, 0:cols], tk[32:64] + lk[0:32]], axis=1) * tau
    left = jnp.concatenate([top[0:32, 0:cols], tk[0:32]], axis=1)
    right = jnp.concatenate([low[32:64, 0:cols], lk[32:64]], axis=1)
    weights = (pltpu.roll(tc[32:64], LANES - 32, 1) + lc[0:32]) * tau
    mid = solve([mid[8 * q : 8 * q + 8] for q in range(4)], weights)
    left = spread(left, tc, 0, mid, 32)
    right = spread(right, lc, 32, mid, 0)

    def ordered(block):
        tile = block[:, cols:]
        at = lane_of(tile.shape)
        swapped = jnp.where(at < 32, pltpu.roll(tile, 96, 1), pltpu.roll(tile, 32, 1))
        return jnp.where(at < 64, jnp.where(even, swapped, tile), 0.0)

    spot = lane_of((32, LANES)) == 64
    left = jnp.concatenate([left[:, 0:cols], jnp.where(spot, tc[0:32, 64:65], ordered(left))], axis=1)
    right = jnp.concatenate([right[:, 0:cols], jnp.where(spot, lc[32:64, 64:65], ordered(right))], axis=1)
    mid_ref[...] = jnp.concatenate([mid[:, 0:cols], ordered(mid)], axis=1)
    e_ref[...] = jnp.where(even, right, left)
    o_ref[...] = jnp.where(even, left, right)


def pair_kernel(e_ref, o_ref, got_ref, pair_ref, p_ref, msg_ref):
    cols = e_ref.shape[1] - LANES
    mine, theirs = e_ref[:, cols:], got_ref[:, cols:]
    tau = 2.0 / (mine[:, 64:65] + theirs[:, 64:65])
    lower = tau * (mine + theirs)
    lane = lane_of(mine.shape)
    upper = (lane >= 32) & (lane < 64)
    outer = to_low(theirs) + jnp.where(upper, mine, 0.0)
    pair = jnp.concatenate([e_ref[:, 0:cols] + got_ref[:, 0:cols], outer], axis=1) * tau
    pair = solve([pair[8 * q : 8 * q + 8] for q in range(4)], lower)
    pair_ref[...] = pair
    tile = o_ref[:, cols:]
    p = jnp.concatenate([o_ref[:, 0:cols], jnp.where((lane >= 32) & (lane < 65), tile, 0.0)], axis=1)
    p = spread(p, tile, 0, pair, 0)
    p_ref[...] = p
    msg_ref[...] = jnp.concatenate([p[0:16], p[16:32, cols:]], axis=1)


def outer_kernel(got_ref, pair_ref, w_ref):
    cols = got_ref.shape[1] - LANES
    tile = got_ref[:, cols:]
    kept = to_low(tile) + jnp.where(lane_of(tile.shape) == 64, tile, 0.0)
    w = jnp.concatenate([got_ref[:, 0:cols], kept], axis=1)
    w_ref[...] = spread(w, tile, 0, pair_ref[...], 0)


def p0_kernel(msg_ref, p_ref, w_ref, p0_ref, scaled_ref, out_ref):
    cols = p_ref.shape[1] - LANES
    got = msg_ref[...]
    both = p_ref[:, cols:] + jnp.concatenate([got[:, cols : cols + LANES], got[:, cols + LANES :]], axis=0)
    tau = 2.0 / both[:, 64:65]
    lower = tau * both
    scaled_ref[...] = jnp.where(lane_of(lower.shape) == 64, tau, lower)
    p0 = substitute((p_ref[0:16, 0:cols] + got[:, 0:cols]) * tau[0:16], lower, 0, 32)
    p0_ref[...] = p0
    tile = w_ref[:, cols:]
    out_ref[...] = jnp.concatenate(
        [jnp.concatenate([w_ref[0:16, 0:cols], spread(w_ref[16:32, 0:cols], tile, 16, p0, 32)], axis=0), tile], axis=1
    )


def w_kernel(msg_ref, start_ref, w_ref, p_ref, p0_ref, out_w_ref, out_ref):
    cols = w_ref.shape[1] - LANES
    chip = chip_of()
    chips = lax.axis_size("rows") // 2
    start = start_ref[:, 0:1]
    valid = (chip != 1) & ((chip != chips - 2) | (start == 0.0))
    both = w_ref[:, cols:] + msg_ref[:, cols:]
    tau = jnp.where(valid, 2.0 / jnp.where(valid, both[:, 64:65], 1.0), 0.0)
    w = (w_ref[:, 0:cols] + msg_ref[:, 0:cols]) * tau
    w = solve([w[8 * q : 8 * q + 8] for q in range(4)], tau * both)
    out_w_ref[...] = w
    tile = p_ref[:, cols:]
    rest = spread(p_ref[16:32, 0:cols], tile, 16, p0_ref[...], 32)
    out_ref[...] = spread(rest, tile, 16, w[0:16], 0)


def known_kernel(pair_ref, w_ref, p0_ref, out_ref):
    cols = w_ref.shape[1]
    tile = pair_ref[:, cols:]
    out_ref[...] = spread(spread(pair_ref[:, 0:cols], tile, 0, w_ref[...], 0), tile, 0, p0_ref[...], 32)


def p1_kernel(msg_ref, scaled_ref, rest_ref, pair_ref, known_ref, p0_ref, p_ref, e_ref):
    cols = msg_ref.shape[1]
    scaled = scaled_ref[...]
    p1 = substitute((rest_ref[...] + msg_ref[...]) * scaled[16:32, 64:65], scaled, 16, 32)
    p_ref[...] = jnp.concatenate([p0_ref[...], p1], axis=0)
    e_ref[...] = spread(known_ref[...], pair_ref[:, cols:], 0, p1, 48)


def inside():
    place = chip_of() % 4
    return (place == 1) | (place == 2)


def mid_kernel(mid_ref, p_ref, got_ref, o_ref, out_ref):
    cols = p_ref.shape[1]
    o = jnp.where(inside(), p_ref[...], got_ref[...])
    o_ref[...] = o
    out_ref[...] = spread(mid_ref[:, 0:cols], mid_ref[:, cols:], 0, o, 32)


def back_kernel(mid_ref, part_ref, o_ref, e_ref, got_ref, keep_ref, out_ref):
    cols = e_ref.shape[1]
    even = chip_of() % 2 == 0
    e, o = jnp.where(inside(), e_ref[...], got_ref[...]), o_ref[...]
    mid = spread(part_ref[...], mid_ref[:, cols:], 0, e, 0)
    out_ref[...] = jnp.concatenate([jnp.where(even, o, e), mid], axis=0)
    keep_ref[...] = jnp.concatenate([mid, jnp.where(even, e, o)], axis=0)


def inner_kernel(inner_ref, proj_ref, high_ref, low_ref, x_ref, y_ref):
    part = dot3(proj_ref[...], (high_ref[...], low_ref[...]))
    y_ref[...] = x_ref[...] - dot3(inner_ref[...], part, ((0,), (0,)))


def final_kernel(edge_ref, keep_ref, msg_ref, y_ref, out_ref):
    south = lax.axis_index("rows") % 2 == 0
    w = jnp.where(south, msg_ref[...], keep_ref[...])
    out_ref[...] = y_ref[...] - dot3(edge_ref[...], w, ((0,), (0,)))


def per_device(eigvecs, reflectors, starts):
    count = lax.axis_size("rows")
    chips = count // 2
    rows, cols = eigvecs.shape
    wide = cols + LANES

    def north(pairs):
        return [(2 * a + 1, 2 * b + 1) for a, b in pairs]

    up = [(2 * c, 2 * c + 1) for c in range(chips)]
    down = [(b, a) for a, b in up]
    to_inner = north([(q, q + 1) for q in range(0, chips, 4)] + [(q + 3, q + 2) for q in range(0, chips, 4)])
    to_outer = [(b, a) for a, b in to_inner]
    p_pairs = north([(q + 1, q + 2) for q in range(0, chips, 4)] + [(q + 2, q + 1) for q in range(0, chips, 4)])
    w_pairs = north([(q + 2, q + 5) for q in range(0, chips - 4, 4)] + [(q + 5, q + 2) for q in range(0, chips - 4, 4)])
    other = lax.ppermute(reflectors, "cols", [(0, 1), (1, 0)])
    half = jax.ShapeDtypeStruct(eigvecs.shape, jnp.bfloat16)
    high, low, own, start = call(
        ready_kernel, [half, half, reflectors.shape, (SWEEPS, LANES)], eigvecs, reflectors, starts[None, :], flops=20_000_000
    )
    msg, inner, proj, edge = call(
        factor_kernel,
        [(64, wide), (96, rows), (96, rows), (64, rows)],
        own, other, start, high, low,
    )
    got = lax.ppermute(msg, "rows", up)
    mid, e, o = call(merge_kernel, [(32, wide)] * 3, msg, got)
    got_e = lax.ppermute(e, "rows", to_inner)
    got_o = lax.ppermute(o, "rows", to_inner)
    pair, p, msg = call(pair_kernel, [(32, wide), (32, wide), (16, wide + LANES)], e, o, got_e)
    got = lax.ppermute(msg, "rows", p_pairs)
    (w,) = call(outer_kernel, [(32, wide)], got_o, pair)
    p0, scaled, w = call(p0_kernel, [(16, cols), (32, LANES), (32, wide)], got, p, w)
    got = lax.ppermute(w, "rows", w_pairs)
    (partial,) = call(inner_kernel, [(rows, cols)], inner, proj, high, low, eigvecs, flops=20_000_000)
    w, rest = call(w_kernel, [(32, cols), (16, cols)], got, start, w, p, p0)
    got = lax.ppermute(rest, "rows", p_pairs)
    got_w = lax.ppermute(w, "rows", to_outer)
    (known,) = call(known_kernel, [(32, cols)], pair, w, p0)
    p, e = call(p1_kernel, [(32, cols), (32, cols)], got, scaled, rest, pair, known, p0)
    got_e = lax.ppermute(e, "rows", to_outer)
    o, part = call(mid_kernel, [(32, cols), (32, cols)], mid, p, got_w)
    keep, msg = call(back_kernel, [(64, cols), (64, cols)], mid, part, o, e, got_e)
    got = lax.ppermute(msg, "rows", down)
    (out,) = call(final_kernel, [(rows, cols)], edge, keep, got, partial)
    return out


def solution(mesh):
    in_specs = (P("rows", "cols"), P("cols", "rows"), P())
    out_specs = P("rows", "cols")
    return jax.shard_map(
        per_device, mesh=mesh, in_specs=in_specs, out_specs=out_specs, check_vma=False
    )
```

```python
import jax
import jax.numpy as jnp
from jax import lax
from jax.experimental import pallas as pl
from jax.experimental.pallas import tpu as pltpu
from jax.sharding import PartitionSpec as P

BAND = 64
SWEEPS = 32
LANES = 128


def dot(a, b, contract=((1,), (0,))):
    return lax.dot_general(
        a, b, (contract, ((), ())), precision=lax.Precision.HIGHEST, preferred_element_type=jnp.float32
    )


def lane_of(shape):
    return lax.broadcasted_iota(jnp.int32, shape, len(shape) - 1)


def row_of(shape):
    return lax.broadcasted_iota(jnp.int32, shape, 0)


def call(kernel, outs, *args, flops=1_000_000):
    nbytes = 4 * sum(a.size for a in args)
    return pl.pallas_call(
        kernel,
        out_shape=[jax.ShapeDtypeStruct(s, jnp.float32) if isinstance(s, tuple) else s for s in outs],
        in_specs=[pl.BlockSpec(memory_space=pltpu.VMEM)] * len(args),
        out_specs=[pl.BlockSpec(memory_space=pltpu.VMEM)] * len(outs),
        compiler_params=pltpu.CompilerParams(vmem_limit_bytes=16 * 1024 * 1024),
        cost_estimate=pl.CostEstimate(flops=flops, bytes_accessed=nbytes, transcendentals=0),
    )(*args)


def split(a):
    high = a.astype(jnp.bfloat16)
    return high, (a - high.astype(jnp.float32)).astype(jnp.bfloat16)


def dot3(a, b, contract=((1,), (0,))):
    (ah, al), (bh, bl) = split(a), b if isinstance(b, tuple) else split(b)

    def one(x, y):
        return lax.dot_general(x, y, (contract, ((), ())), preferred_element_type=jnp.float32)

    return one(ah, bh) + (one(ah, bl) + one(al, bh))


def ready_kernel(x_ref, own_ref, start_ref, high_ref, low_ref, copy_ref, column_ref):
    high_ref[...], low_ref[...] = split(x_ref[...])
    copy_ref[...] = own_ref[...]
    square = (SWEEPS, SWEEPS)
    row = start_ref[...].astype(jnp.float32)
    column = jnp.sum(jnp.where(lane_of(square) == row_of(square), row, 0.0), axis=1, keepdims=True)
    column_ref[...] = jnp.broadcast_to(column, (SWEEPS, LANES))


def factor_kernel(own_ref, other_ref, start_ref, high_ref, low_ref, msg_ref, inner_ref, proj_ref, edge_ref):
    first = lax.axis_index("cols") == 0
    own, other = own_ref[...], other_ref[...]
    r = jnp.concatenate([jnp.where(first, own, other), jnp.where(first, other, own)], axis=0)
    rows = r.shape[1]
    start = start_ref[:, 0:1].astype(jnp.int32)
    segment = (lane_of(r.shape) - start + BAND) >> 6
    parts = [jnp.where(segment == k, r, 0.0) for k in range(5)]
    zero = jnp.zeros_like(r)
    inner = jnp.concatenate(parts[1:4], axis=0)
    edge = jnp.concatenate([parts[0], parts[4]], axis=0)
    left = jnp.concatenate([inner, zero, edge], axis=0)
    right = jnp.concatenate([inner, zero, edge, zero, zero], axis=0)
    gram = dot(left, right, ((1,), (1,)))
    earlier = (lane_of(gram.shape) & (SWEEPS - 1)) < (row_of(gram.shape) & (SWEEPS - 1))
    gram = jnp.where(earlier, gram, 0.0)
    count = 3 * SWEEPS
    tau = 2.0 / jnp.sum(inner * inner, axis=1, keepdims=True)
    lower = tau * gram[0:count, 0:LANES]
    rhs = tau * jnp.concatenate([inner, gram[0:count, LANES : 2 * LANES]], axis=1)
    blocks = [[rhs[32 * k + 8 * q : 32 * k + 8 * q + 8] for q in range(4)] for k in range(3)]
    for j in range(SWEEPS - 1):
        source = [blocks[k][j // 8][j % 8 : j % 8 + 1] for k in range(3)]
        for k in range(3):
            for q in range((j + 1) // 8, 4):
                at = 32 * k + 8 * q
                total = blocks[k][q]
                for m in range(3):
                    if abs(m - k) < 2:
                        column = 32 * m + j
                        total = total - lower[at : at + 8, column : column + 1] * source[m]
                blocks[k][q] = total
    solved = jnp.concatenate([blocks[k][q] for k in range(3) for q in range(4)] + [jnp.zeros((32, rhs.shape[1]), jnp.float32)], axis=0)
    back = dot(gram[LANES : LANES + 64, 0:LANES], solved)
    observe = edge - back[:, 0:rows]
    couple = back[:, rows:] - gram[LANES : LANES + 64, LANES : 2 * LANES]
    squares = jnp.sum(edge * edge, axis=1, keepdims=True)
    coef = jnp.where(lane_of(couple.shape) == 64, squares, couple)
    inner_ref[...] = inner
    proj_ref[...] = solved[0:count, 0:rows]
    edge_ref[...] = edge - dot(solved[0:count, rows : rows + 64], inner, ((0,), (0,)))
    msg_ref[...] = jnp.concatenate([dot3(observe, (high_ref[...], low_ref[...])), coef], axis=1)


def to_low(tile):
    return jnp.where(lane_of(tile.shape) < 32, pltpu.roll(tile, LANES - 32, 1), 0.0)


def solve(blocks, lower, lane=0):
    for j in range(SWEEPS):
        source = blocks[j // 8][j % 8 : j % 8 + 1]
        for q in range((j + 1) // 8, len(blocks)):
            blocks[q] = blocks[q] + lower[8 * q : 8 * q + 8, lane + j : lane + j + 1] * source
    return jnp.concatenate(blocks, axis=0)


def spread(rows, tile, at, solved, lane):
    for j in range(solved.shape[0]):
        rows = rows + tile[at : at + rows.shape[0], lane + j : lane + j + 1] * solved[j : j + 1]
    return rows


def substitute(block, lower, first, lane):
    for j in range(block.shape[0] - 1):
        block = block + lower[first : first + block.shape[0], lane + first + j : lane + first + j + 1] * block[j : j + 1]
    return block


def chip_of():
    return lax.axis_index("rows") // 2


def merge_kernel(own_ref, got_ref, mid_ref, e_ref, o_ref):
    even = chip_of() % 2 == 0
    cols = own_ref.shape[1] - LANES
    top, low = got_ref[...], own_ref[...]
    tc, lc = top[:, cols:], low[:, cols:]
    tau = 2.0 / (tc[32:64, 64:65] + lc[0:32, 64:65])
    lane = lane_of(tc.shape)
    tk = jnp.where(lane < 32, tc, 0.0)
    lk = jnp.where((lane >= 32) & (lane < 64), lc, 0.0)
    mid = jnp.concatenate([top[32:64, 0:cols] + low[0:32, 0:cols], tk[32:64] + lk[0:32]], axis=1) * tau
    left = jnp.concatenate([top[0:32, 0:cols], tk[0:32]], axis=1)
    right = jnp.concatenate([low[32:64, 0:cols], lk[32:64]], axis=1)
    weights = (pltpu.roll(tc[32:64], LANES - 32, 1) + lc[0:32]) * tau
    mid = solve([mid[8 * q : 8 * q + 8] for q in range(4)], weights)
    left = spread(left, tc, 0, mid, 32)
    right = spread(right, lc, 32, mid, 0)

    def ordered(block):
        tile = block[:, cols:]
        at = lane_of(tile.shape)
        swapped = jnp.where(at < 32, pltpu.roll(tile, 96, 1), pltpu.roll(tile, 32, 1))
        return jnp.where(at < 64, jnp.where(even, swapped, tile), 0.0)

    spot = lane_of((32, LANES)) == 64
    left = jnp.concatenate([left[:, 0:cols], jnp.where(spot, tc[0:32, 64:65], ordered(left))], axis=1)
    right = jnp.concatenate([right[:, 0:cols], jnp.where(spot, lc[32:64, 64:65], ordered(right))], axis=1)
    mid_ref[...] = jnp.concatenate([mid[:, 0:cols], ordered(mid)], axis=1)
    e_ref[...] = jnp.where(even, right, left)
    o_ref[...] = jnp.where(even, left, right)


def pair_kernel(e_ref, o_ref, got_ref, pair_ref, p_ref, msg_ref):
    cols = e_ref.shape[1] - LANES
    mine, theirs = e_ref[:, cols:], got_ref[:, cols:]
    tau = 2.0 / (mine[:, 64:65] + theirs[:, 64:65])
    lower = tau * (mine + theirs)
    lane = lane_of(mine.shape)
    upper = (lane >= 32) & (lane < 64)
    outer = to_low(theirs) + jnp.where(upper, mine, 0.0)
    pair = jnp.concatenate([e_ref[:, 0:cols] + got_ref[:, 0:cols], outer], axis=1) * tau
    pair = solve([pair[8 * q : 8 * q + 8] for q in range(4)], lower)
    pair_ref[...] = pair
    tile = o_ref[:, cols:]
    p = jnp.concatenate([o_ref[:, 0:cols], jnp.where((lane >= 32) & (lane < 65), tile, 0.0)], axis=1)
    p = spread(p, tile, 0, pair, 0)
    p_ref[...] = p
    msg_ref[...] = jnp.concatenate([p[0:16], p[16:32, cols:]], axis=1)


def outer_kernel(got_ref, pair_ref, w_ref):
    cols = got_ref.shape[1] - LANES
    tile = got_ref[:, cols:]
    kept = to_low(tile) + jnp.where(lane_of(tile.shape) == 64, tile, 0.0)
    w = jnp.concatenate([got_ref[:, 0:cols], kept], axis=1)
    w_ref[...] = spread(w, tile, 0, pair_ref[...], 0)


def p0_kernel(msg_ref, p_ref, w_ref, p0_ref, scaled_ref, out_ref):
    cols = p_ref.shape[1] - LANES
    got = msg_ref[...]
    both = p_ref[:, cols:] + jnp.concatenate([got[:, cols : cols + LANES], got[:, cols + LANES :]], axis=0)
    tau = 2.0 / both[:, 64:65]
    lower = tau * both
    scaled_ref[...] = jnp.where(lane_of(lower.shape) == 64, tau, lower)
    p0 = substitute((p_ref[0:16, 0:cols] + got[:, 0:cols]) * tau[0:16], lower, 0, 32)
    p0_ref[...] = p0
    tile = w_ref[:, cols:]
    out_ref[...] = jnp.concatenate(
        [jnp.concatenate([w_ref[0:16, 0:cols], spread(w_ref[16:32, 0:cols], tile, 16, p0, 32)], axis=0), tile], axis=1
    )


def w_kernel(msg_ref, start_ref, w_ref, p_ref, p0_ref, out_w_ref, out_ref):
    cols = w_ref.shape[1] - LANES
    chip = chip_of()
    chips = lax.axis_size("rows") // 2
    start = start_ref[:, 0:1]
    valid = (chip != 1) & ((chip != chips - 2) | (start == 0.0))
    got = jnp.where((chip != 1) & (chip != chips - 2), msg_ref[...], 0.0)
    both = w_ref[:, cols:] + got[:, cols:]
    tau = jnp.where(valid, 2.0 / jnp.where(valid, both[:, 64:65], 1.0), 0.0)
    w = (w_ref[:, 0:cols] + got[:, 0:cols]) * tau
    w = solve([w[8 * q : 8 * q + 8] for q in range(4)], tau * both)
    out_w_ref[...] = w
    tile = p_ref[:, cols:]
    rest = spread(p_ref[16:32, 0:cols], tile, 16, p0_ref[...], 32)
    out_ref[...] = spread(rest, tile, 16, w[0:16], 0)


def known_kernel(pair_ref, w_ref, p0_ref, out_ref):
    cols = w_ref.shape[1]
    tile = pair_ref[:, cols:]
    out_ref[...] = spread(spread(pair_ref[:, 0:cols], tile, 0, w_ref[...], 0), tile, 0, p0_ref[...], 32)


def p1_kernel(msg_ref, scaled_ref, rest_ref, pair_ref, known_ref, p0_ref, p_ref, e_ref):
    cols = msg_ref.shape[1]
    scaled = scaled_ref[...]
    p1 = substitute((rest_ref[...] + msg_ref[...]) * scaled[16:32, 64:65], scaled, 16, 32)
    p_ref[...] = jnp.concatenate([p0_ref[...], p1], axis=0)
    e_ref[...] = spread(known_ref[...], pair_ref[:, cols:], 0, p1, 48)


def inside():
    place = chip_of() % 4
    return (place == 1) | (place == 2)


def mid_kernel(mid_ref, p_ref, got_ref, o_ref, out_ref):
    cols = p_ref.shape[1]
    o = jnp.where(inside(), p_ref[...], got_ref[...])
    o_ref[...] = o
    out_ref[...] = spread(mid_ref[:, 0:cols], mid_ref[:, cols:], 0, o, 32)


def back_kernel(mid_ref, part_ref, o_ref, e_ref, got_ref, keep_ref, out_ref):
    cols = e_ref.shape[1]
    even = chip_of() % 2 == 0
    e, o = jnp.where(inside(), e_ref[...], got_ref[...]), o_ref[...]
    mid = spread(part_ref[...], mid_ref[:, cols:], 0, e, 0)
    out_ref[...] = jnp.concatenate([jnp.where(even, o, e), mid], axis=0)
    keep_ref[...] = jnp.concatenate([mid, jnp.where(even, e, o)], axis=0)


def inner_kernel(inner_ref, proj_ref, high_ref, low_ref, x_ref, y_ref):
    part = dot3(proj_ref[...], (high_ref[...], low_ref[...]))
    y_ref[...] = x_ref[...] - dot3(inner_ref[...], part, ((0,), (0,)))


def final_kernel(edge_ref, keep_ref, msg_ref, y_ref, out_ref, piece_ref, sems):
    south = lax.axis_index("rows") % 2 == 0
    edge = edge_ref[...]
    pieces = piece_ref.shape[0]
    width = piece_ref.shape[2]
    copies = []
    for i in range(pieces):
        at = slice(i * width, (i + 1) * width)
        w = jnp.where(south, msg_ref[:, at], keep_ref[:, at])
        piece_ref[i] = y_ref[:, at] - dot3(edge, w, ((0,), (0,)))
        copy = pltpu.make_async_copy(piece_ref.at[i], out_ref.at[:, at], sems.at[i])
        copy.start()
        copies.append(copy)
    for copy in copies:
        copy.wait()


def per_device(eigvecs, reflectors, starts):
    count = lax.axis_size("rows")
    chips = count // 2
    rows, cols = eigvecs.shape
    wide = cols + LANES

    def place_of(i):
        return i % 2 == 1, (i // 2) % 4 in (1, 2), (i // 2) % 4 == 2

    def swap(pick):
        return [(i, pick(i, *place_of(i)) % count) for i in range(count)]

    on_chip = swap(lambda i, north, inside, last: i ^ 1)
    in_pair = swap(lambda i, north, inside, last: i ^ 2 if north else i ^ 8)
    p_pairs = swap(lambda i, north, inside, last: i ^ 6 if north and inside else i ^ 8)
    w_pairs = swap(lambda i, north, inside, last: (i + 6 if last else i - 6) if north and inside else i ^ 8 if north else i ^ 2)
    other = lax.ppermute(reflectors, "cols", [(0, 1), (1, 0)])
    half = jax.ShapeDtypeStruct(eigvecs.shape, jnp.bfloat16)
    high, low, own, start = call(
        ready_kernel, [half, half, reflectors.shape, (SWEEPS, LANES)], eigvecs, reflectors, starts[None, :], flops=20_000_000
    )
    msg, inner, proj, edge = call(
        factor_kernel,
        [(64, wide), (96, rows), (96, rows), (64, rows)],
        own, other, start, high, low,
    )
    got = lax.ppermute(msg, "rows", on_chip)
    mid, e, o = call(merge_kernel, [(32, wide)] * 3, msg, got)
    got_e = lax.ppermute(e, "rows", in_pair)
    got_o = lax.ppermute(o, "rows", in_pair)
    pair, p, msg = call(pair_kernel, [(32, wide), (32, wide), (16, wide + LANES)], e, o, got_e)
    got = lax.ppermute(msg, "rows", p_pairs)
    (w,) = call(outer_kernel, [(32, wide)], got_o, pair)
    p0, scaled, w = call(p0_kernel, [(16, cols), (32, LANES), (32, wide)], got, p, w)
    got = lax.ppermute(w, "rows", w_pairs)
    (partial,) = call(inner_kernel, [(rows, cols)], inner, proj, high, low, eigvecs, flops=20_000_000)
    w, rest = call(w_kernel, [(32, cols), (16, cols)], got, start, w, p, p0)
    got = lax.ppermute(rest, "rows", p_pairs)
    got_w = lax.ppermute(w, "rows", in_pair)
    (known,) = call(known_kernel, [(32, cols)], pair, w, p0)
    p, e = call(p1_kernel, [(32, cols), (32, cols)], got, scaled, rest, pair, known, p0)
    got_e = lax.ppermute(e, "rows", in_pair)
    o, part = call(mid_kernel, [(32, cols), (32, cols)], mid, p, got_w)
    keep, msg = call(back_kernel, [(64, cols), (64, cols)], mid, part, o, e, got_e)
    got = lax.ppermute(msg, "rows", on_chip)
    return pl.pallas_call(
        final_kernel,
        out_shape=jax.ShapeDtypeStruct((rows, cols), jnp.float32),
        in_specs=[pl.BlockSpec(memory_space=pltpu.VMEM)] * 4,
        out_specs=pl.BlockSpec(memory_space=pl.ANY),
        scratch_shapes=[pltpu.VMEM((4, rows, cols // 4), jnp.float32), pltpu.SemaphoreType.DMA((4,))],
        compiler_params=pltpu.CompilerParams(vmem_limit_bytes=16 * 1024 * 1024),
    )(edge, keep, got, partial)


def solution(mesh):
    in_specs = (P("rows", "cols"), P("cols", "rows"), P())
    out_specs = P("rows", "cols")
    return jax.shard_map(
        per_device, mesh=mesh, in_specs=in_specs, out_specs=out_specs, check_vma=False
    )
```

```python
import jax
import jax.numpy as jnp
from jax import lax
from jax.experimental import pallas as pl
from jax.experimental.pallas import tpu as pltpu
from jax.sharding import PartitionSpec as P


BAND = 64
SWEEPS = 32
LANES = 128


def dot(a, b, contract=((1,), (0,))):
    return lax.dot_general(
        a, b, (contract, ((), ())), precision=lax.Precision.HIGHEST, preferred_element_type=jnp.float32
    )


def lane_of(shape):
    return lax.broadcasted_iota(jnp.int32, shape, len(shape) - 1)


def row_of(shape):
    return lax.broadcasted_iota(jnp.int32, shape, 0)


def call(kernel, outs, *args, where=None, flops=1_000_000):
    def body(*refs):
        if where is None:
            kernel(*refs)
        else:
            pl.when(where())(lambda: kernel(*refs))

    nbytes = 4 * sum(a.size for a in args)
    return pl.pallas_call(
        body,
        out_shape=[jax.ShapeDtypeStruct(s, jnp.float32) if isinstance(s, tuple) else s for s in outs],
        in_specs=[pl.BlockSpec(memory_space=pltpu.VMEM)] * len(args),
        out_specs=[pl.BlockSpec(memory_space=pltpu.VMEM)] * len(outs),
        compiler_params=pltpu.CompilerParams(vmem_limit_bytes=16 * 1024 * 1024),
        cost_estimate=pl.CostEstimate(flops=flops, bytes_accessed=nbytes, transcendentals=0),
    )(*args)


def chip_of():
    return lax.axis_index("rows") // 2


def is_north():
    return lax.axis_index("rows") % 2 == 1


def is_inside():
    index = lax.axis_index("rows")
    place = (index // 2) % 4
    return (index % 2 == 1) & ((place == 1) | (place == 2))


def split(a):
    high = a.astype(jnp.bfloat16)
    return high, (a - high.astype(jnp.float32)).astype(jnp.bfloat16)


def dot3(a, b, contract=((1,), (0,))):
    (ah, al), (bh, bl) = split(a), b if isinstance(b, tuple) else split(b)

    def one(x, y):
        return lax.dot_general(x, y, (contract, ((), ())), preferred_element_type=jnp.float32)

    return one(ah, bh) + (one(ah, bl) + one(al, bh))


def ready_kernel(x_ref, start_ref, high_ref, low_ref, column_ref):
    high_ref[...], low_ref[...] = split(x_ref[...])
    square = (SWEEPS, SWEEPS)
    row = start_ref[...].astype(jnp.float32)
    column = jnp.sum(jnp.where(lane_of(square) == row_of(square), row, 0.0), axis=1, keepdims=True)
    column_ref[...] = jnp.broadcast_to(column, (SWEEPS, LANES))


def factor_kernel(own_ref, other_ref, start_ref, high_ref, low_ref, msg_ref, inner_ref, edge_ref, solved_ref):
    first = lax.axis_index("cols") == 0
    own, other = own_ref[...], other_ref[...]
    r = jnp.concatenate([jnp.where(first, own, other), jnp.where(first, other, own)], axis=0)
    rows = r.shape[1]
    start = start_ref[:, 0:1].astype(jnp.int32)
    segment = (lane_of(r.shape) - start + BAND) >> 6
    parts = [jnp.where(segment == k, r, 0.0) for k in range(5)]
    zero = jnp.zeros_like(r)
    inner = jnp.concatenate(parts[1:4], axis=0)
    edge = jnp.concatenate([parts[0], parts[4]], axis=0)
    left = jnp.concatenate([inner, zero, edge], axis=0)
    right = jnp.concatenate([inner, zero, edge, zero, zero], axis=0)
    gram = dot3(left, right, ((1,), (1,)))
    earlier = (lane_of(gram.shape) & (SWEEPS - 1)) < (row_of(gram.shape) & (SWEEPS - 1))
    gram = jnp.where(earlier, gram, 0.0)
    count = 3 * SWEEPS
    tau = 2.0 / jnp.sum(inner * inner, axis=1, keepdims=True)
    lower = tau * gram[0:count, 0:LANES]
    rhs = tau * jnp.concatenate([inner, gram[0:count, LANES : 2 * LANES]], axis=1)
    blocks = [[rhs[32 * k + 8 * q : 32 * k + 8 * q + 8] for q in range(4)] for k in range(3)]
    for j in range(SWEEPS - 1):
        source = [blocks[k][j // 8][j % 8 : j % 8 + 1] for k in range(3)]
        for k in range(3):
            for q in range((j + 1) // 8, 4):
                at = 32 * k + 8 * q
                total = blocks[k][q]
                for m in range(3):
                    if abs(m - k) < 2:
                        column = 32 * m + j
                        total = total - lower[at : at + 8, column : column + 1] * source[m]
                blocks[k][q] = total
    solved = jnp.concatenate([blocks[k][q] for k in range(3) for q in range(4)] + [jnp.zeros((32, rhs.shape[1]), jnp.float32)], axis=0)
    back = dot3(gram[LANES : LANES + 64, 0:LANES], solved)
    observe = edge - back[:, 0:rows]
    couple = back[:, rows:] - gram[LANES : LANES + 64, LANES : 2 * LANES]
    squares = jnp.sum(edge * edge, axis=1, keepdims=True)
    coef = jnp.where(lane_of(couple.shape) == 64, squares, couple)
    inner_ref[...] = inner
    edge_ref[...] = edge
    solved_ref[...] = solved[0:count]
    msg_ref[...] = jnp.concatenate([dot3(observe, (high_ref[...], low_ref[...])), coef], axis=1)


def to_low(tile):
    return jnp.where(lane_of(tile.shape) < 32, pltpu.roll(tile, LANES - 32, 1), 0.0)


def solve(blocks, lower, lane=0):
    for j in range(SWEEPS):
        source = blocks[j // 8][j % 8 : j % 8 + 1]
        for q in range((j + 1) // 8, len(blocks)):
            blocks[q] = blocks[q] + lower[8 * q : 8 * q + 8, lane + j : lane + j + 1] * source
    return jnp.concatenate(blocks, axis=0)


def spread(rows, tile, at, solved, lane, first=0, reach=1):
    blocks = [rows[8 * q : 8 * q + 8] for q in range(rows.shape[0] // 8)]
    for j in range(solved.shape[0]):
        for q in range(len(blocks)):
            top = at + 8 * q
            if top + 7 >= first + j + reach:
                column = lane + first + j
                blocks[q] = blocks[q] + tile[top : top + 8, column : column + 1] * solved[j : j + 1]
    return blocks[0] if len(blocks) == 1 else jnp.concatenate(blocks, axis=0)


def substitute(block, lower, first, lane):
    for j in range(block.shape[0] - 1):
        block = block + lower[first : first + block.shape[0], lane + first + j : lane + first + j + 1] * block[j : j + 1]
    return block


def merge_kernel(own_ref, got_ref, mid_ref, first_ref, rest_ref):
    even = chip_of() % 2 == 0
    cols = own_ref.shape[1] - LANES
    top, low = got_ref[...], own_ref[...]
    tc, lc = top[:, cols:], low[:, cols:]
    tau = 2.0 / (tc[32:64, 64:65] + lc[0:32, 64:65])
    lane = lane_of(tc.shape)
    tk = jnp.where(lane < 32, tc, 0.0)
    lk = jnp.where((lane >= 32) & (lane < 64), lc, 0.0)
    mid = jnp.concatenate([top[32:64, 0:cols] + low[0:32, 0:cols], tk[32:64] + lk[0:32]], axis=1) * tau
    left = jnp.concatenate([top[0:32, 0:cols], tk[0:32]], axis=1)
    right = jnp.concatenate([low[32:64, 0:cols], lk[32:64]], axis=1)
    weights = (pltpu.roll(tc[32:64], LANES - 32, 1) + lc[0:32]) * tau
    mid = solve([mid[8 * q : 8 * q + 8] for q in range(4)], weights)
    left = spread(left, tc[0:32], 0, mid, 32, reach=4)
    right = spread(right, lc[32:64], 0, mid, 0, reach=4)

    def ordered(block):
        tile = block[:, cols:]
        at = lane_of(tile.shape)
        swapped = jnp.where(at < 32, pltpu.roll(tile, 96, 1), pltpu.roll(tile, 32, 1))
        return jnp.where(at < 64, jnp.where(even, swapped, tile), 0.0)

    spot = lane_of((32, LANES)) == 64
    left = jnp.concatenate([left[:, 0:cols], jnp.where(spot, tc[0:32, 64:65], ordered(left))], axis=1)
    right = jnp.concatenate([right[:, 0:cols], jnp.where(spot, lc[32:64, 64:65], ordered(right))], axis=1)
    mid_ref[...] = jnp.concatenate([mid[:, 0:cols], ordered(mid)], axis=1)
    e = jnp.where(even, right, left)
    first_ref[...] = e[0:8]
    rest_ref[...] = jnp.concatenate([e[8:32], jnp.where(even, left, right)], axis=0)


def pair_kernel(first_ref, rest_ref, got_ref, msg_ref):
    cols = first_ref.shape[1] - LANES
    both = first_ref[...] + got_ref[...]
    tau = 2.0 / both[:, cols + 64 : cols + 65]
    e = substitute(both[:, 0:cols] * tau, tau * both[:, cols:], 0, 0)
    tile = rest_ref[24:56, cols:]
    p = spread(rest_ref[24:40, 0:cols], tile, 0, e, 0, reach=8)
    msg_ref[...] = jnp.concatenate([p, tile[0:16], tile[16:32]], axis=1)


def edges_kernel(first_ref, rest_ref, got_first_ref, got_rest_ref, pair_ref, p_ref, w_ref):
    cols = first_ref.shape[1] - LANES
    own = jnp.concatenate([first_ref[...], rest_ref[0:24]], axis=0)
    got = jnp.concatenate([got_first_ref[...], got_rest_ref[0:24]], axis=0)
    mine, theirs = own[:, cols:], got[:, cols:]
    tau = 2.0 / (mine[:, 64:65] + theirs[:, 64:65])
    lane = lane_of(mine.shape)
    upper = (lane >= 32) & (lane < 64)
    outer = to_low(theirs) + jnp.where(upper, mine, 0.0)
    pair = jnp.concatenate([own[:, 0:cols] + got[:, 0:cols], outer], axis=1) * tau
    pair = solve([pair[8 * q : 8 * q + 8] for q in range(4)], tau * (mine + theirs))
    pair_ref[...] = pair
    tile = rest_ref[40:56, cols:]
    p = jnp.concatenate([rest_ref[40:56, 0:cols], jnp.where((lane_of(tile.shape) >= 32) & (lane_of(tile.shape) < 64), tile, 0.0)], axis=1)
    p_ref[...] = spread(p, rest_ref[24:56, cols:], 16, pair[0:24], 0, reach=8)
    tile = got_rest_ref[24:56, cols:]
    w = jnp.concatenate([got_rest_ref[24:56, 0:cols], to_low(tile) + jnp.where(lane == 64, tile, 0.0)], axis=1)
    w_ref[...] = spread(w, tile, 0, pair[0:24], 0, reach=8)


def p0_kernel(msg_ref, own_ref, w_ref, p0_ref, scaled_ref, out_ref):
    cols = w_ref.shape[1] - LANES
    both = own_ref[...] + msg_ref[...]
    tile = jnp.concatenate([both[:, cols : cols + LANES], both[:, cols + LANES :]], axis=0)
    tau = 2.0 / tile[:, 64:65]
    lower = tau * tile
    scaled_ref[...] = jnp.where(lane_of(lower.shape) == 64, tau, lower)
    p0 = substitute(both[:, 0:cols] * tau[0:16], lower, 0, 32)
    p0_ref[...] = p0
    tile = w_ref[:, cols:]
    w = jnp.concatenate([w_ref[0:16, 0:cols], spread(w_ref[16:32, 0:cols], tile, 16, p0, 32, reach=16)], axis=0)
    out_ref[...] = jnp.concatenate([w, tile], axis=1)


def w_kernel(msg_ref, start_ref, w_ref, p_ref, p0_ref, out_w_ref, out_ref):
    cols = w_ref.shape[1] - LANES
    chip = chip_of()
    chips = lax.axis_size("rows") // 2
    start = start_ref[:, 0:1]
    valid = (chip != 1) & ((chip != chips - 2) | (start == 0.0))
    got = jnp.where((chip != 1) & (chip != chips - 2), msg_ref[...], 0.0)
    both = w_ref[...] + got
    squares = both[:, cols + 64 : cols + 65]
    tau = jnp.where(valid, 2.0 / jnp.where(valid, squares, 1.0), 0.0)
    w = both[:, 0:cols] * tau
    w = solve([w[8 * q : 8 * q + 8] for q in range(4)], tau * both[:, cols:])
    out_w_ref[...] = w
    tile = jnp.concatenate([p_ref[:, cols:], p_ref[:, cols:]], axis=0)
    rest = spread(p_ref[:, 0:cols], tile, 16, p0_ref[...], 32)
    out_ref[...] = spread(rest, tile, 16, w[0:16], 0, reach=16)


def e0_kernel(pair_ref, w_ref, p0_ref, out_ref, tail_ref):
    cols = w_ref.shape[1]
    tile = pair_ref[:, cols:]
    w = w_ref[...]
    e = spread(pair_ref[:, 0:cols], tile, 0, w[0:24], 0, reach=8)
    e = spread(e, tile, 0, p0_ref[...], 32, reach=8)
    out_ref[...] = jnp.concatenate([w, e[0:24]], axis=0)
    tail_ref[...] = e[24:32]


def p1_kernel(msg_ref, scaled_ref, rest_ref, pair_ref, tail_ref, p0_ref, p_ref, out_ref):
    cols = msg_ref.shape[1]
    scaled = scaled_ref[...]
    p1 = substitute((rest_ref[...] + msg_ref[...]) * scaled[16:32, 64:65], scaled, 16, 32)
    p_ref[...] = jnp.concatenate([p0_ref[...], p1], axis=0)
    out_ref[...] = spread(tail_ref[...], pair_ref[:, cols:], 24, p1[0:8], 32, first=16, reach=8)


def mid_kernel(mid_ref, p_ref, own_ref, got_ref, part_ref, o_ref, e_ref):
    cols = p_ref.shape[1]
    inside = is_inside()
    o = jnp.where(inside, p_ref[...], got_ref[0:32])
    e = jnp.where(inside, own_ref[32:56], got_ref[32:56])
    tile = mid_ref[:, cols:]
    o_ref[...] = o
    e_ref[...] = e
    part_ref[...] = spread(spread(mid_ref[:, 0:cols], tile, 0, e, 0, reach=4), tile, 0, o, 32, reach=4)


def back_kernel(mid_ref, part_ref, o_ref, e_ref, own_ref, got_ref, keep_ref, out_ref):
    cols = o_ref.shape[1]
    even = chip_of() % 2 == 0
    tail = jnp.where(is_inside(), own_ref[...], got_ref[...])
    last = spread(part_ref[24:32], mid_ref[:, cols:], 24, tail, 0, first=24, reach=4)
    for q in range(4):
        at = slice(8 * q, 8 * q + 8)
        below = slice(32 + 8 * q, 40 + 8 * q)
        e = tail if q == 3 else e_ref[at]
        mid = last if q == 3 else part_ref[at]
        o = o_ref[at]
        out_ref[at] = jnp.where(even, o, e)
        out_ref[below] = mid
        keep_ref[at] = mid
        keep_ref[below] = jnp.where(even, e, o)


def inner_kernel(inner_ref, edge_ref, solved_ref, high_ref, low_ref, x_ref, y_ref, lhs_ref):
    rows = x_ref.shape[0]
    inner = inner_ref[...]
    part = dot3(solved_ref[:, 0:rows], (high_ref[...], low_ref[...]))
    y_ref[...] = x_ref[...] - dot3(inner, part, ((0,), (0,)))
    edge = edge_ref[...] - dot(solved_ref[:, rows : rows + 64], inner, ((0,), (0,)))
    high = edge.astype(jnp.bfloat16).astype(jnp.float32)
    stack = jnp.concatenate([high, high, edge - high, jnp.zeros_like(edge)], axis=0)
    lhs_ref[...] = stack.T.astype(jnp.bfloat16)


def final_kernel(lhs_ref, keep_ref, msg_ref, y_ref, out_ref, piece_ref, sems):
    north = is_north()
    lhs = lhs_ref[...]
    width = piece_ref.shape[2]
    copies = []
    for i in range(piece_ref.shape[0]):
        at = slice(i * width, (i + 1) * width)
        high, low = split(jnp.where(north, keep_ref[:, at], msg_ref[:, at]))
        rhs = jnp.concatenate([high, low, high, jnp.zeros_like(high)], axis=0)
        piece_ref[i] = y_ref[:, at] - jnp.dot(lhs, rhs, preferred_element_type=jnp.float32)
        copy = pltpu.make_async_copy(piece_ref.at[i], out_ref.at[:, at], sems.at[i])
        copy.start()
        copies.append(copy)
    for copy in copies:
        copy.wait()


def trade(array, pairs):
    return lax.ppermute(array, "rows", pairs)


def per_device(eigvecs, reflectors, starts):
    count = lax.axis_size("rows")
    chips = count // 2
    rows, cols = eigvecs.shape
    wide = cols + LANES

    far = 32 if count >= 64 else 8

    def swap(pick):
        return [(i, pick(i, i // 2, i % 2 == 1, (i // 2) % 4 in (1, 2))) for i in range(count)]

    def next_quad(i, chip, north, inside):
        end = chip < 2 or chip >= chips - 2
        if end and not inside:
            return None if north else i + 3 if chip == 0 else i - 1
        if north and inside:
            return i - 3 if chip == 1 else i + 1 if end else i + 6 if chip % 4 == 2 else i - 6
        return i ^ far if inside else i ^ 1

    on_chip = swap(lambda i, chip, north, inside: i ^ 1)
    in_pair = swap(lambda i, chip, north, inside: i ^ 2 if north else i ^ 8)
    p_pairs = swap(lambda i, chip, north, inside: (i ^ 6 if north else i ^ 8) if inside else i ^ 1)
    w_pairs = [
        (2 * i + c, 2 * i + 1 - c if j is None else 2 * j + c) for i, j in swap(next_quad) for c in range(2)
    ]
    other = lax.ppermute(reflectors, "cols", [(0, 1), (1, 0)])
    half = jax.ShapeDtypeStruct(eigvecs.shape, jnp.bfloat16)
    high, low, start = call(ready_kernel, [half, half, (SWEEPS, LANES)], eigvecs, starts[None, :], flops=20_000_000)
    msg, inner, edge, solved = call(
        factor_kernel, [(64, wide), (96, rows), (64, rows), (96, rows + LANES)], reflectors, other, start, high, low
    )
    got = lax.ppermute(msg, "rows", on_chip)
    mid, first, rest = call(merge_kernel, [(32, wide), (8, wide), (56, wide)], msg, got, where=is_north)
    got_first = trade(first, in_pair)
    got_rest = trade(rest, in_pair)
    (msg,) = call(pair_kernel, [(16, wide + LANES)], first, rest, got_first, where=is_inside)
    got = lax.ppermute(msg, "rows", p_pairs)
    pair, p, w = call(
        edges_kernel, [(32, wide), (16, wide), (32, wide)], first, rest, got_first, got_rest, where=is_inside
    )
    p0, scaled, w = call(p0_kernel, [(16, cols), (32, LANES), (32, wide)], got, msg, w, where=is_inside)
    got = lax.ppermute(w, ("rows", "cols"), w_pairs)
    partial, lhs = call(
        inner_kernel, [(rows, cols), jax.ShapeDtypeStruct((rows, 256), jnp.bfloat16)],
        inner, edge, solved, high, low, eigvecs, flops=20_000_000,
    )
    w, rest = call(w_kernel, [(32, cols), (16, cols)], got, start, w, p, p0, where=is_inside)
    got = trade(rest, p_pairs)
    most, tail = call(e0_kernel, [(56, cols), (8, cols)], pair, w, p0, where=is_inside)
    got_most = trade(most, in_pair)
    p, tail = call(p1_kernel, [(32, cols), (8, cols)], got, scaled, rest, pair, tail, p0, where=is_inside)
    got = lax.ppermute(tail, "rows", in_pair)
    part, o, e = call(mid_kernel, [(32, cols), (32, cols), (24, cols)], mid, p, most, got_most, where=is_north)
    keep, msg = call(back_kernel, [(64, cols), (64, cols)], mid, part, o, e, tail, got, where=is_north)
    got = lax.ppermute(msg, "rows", on_chip)
    return pl.pallas_call(
        final_kernel,
        out_shape=jax.ShapeDtypeStruct((rows, cols), jnp.float32),
        in_specs=[pl.BlockSpec(memory_space=pltpu.VMEM)] * 4,
        out_specs=pl.BlockSpec(memory_space=pl.ANY),
        scratch_shapes=[pltpu.VMEM((4, rows, cols // 4), jnp.float32), pltpu.SemaphoreType.DMA((4,))],
        compiler_params=pltpu.CompilerParams(vmem_limit_bytes=16 * 1024 * 1024),
    )(lhs, keep, got, partial)


def solution(mesh):
    in_specs = (P("rows", "cols"), P("cols", "rows"), P())
    out_specs = P("rows", "cols")

    return jax.shard_map(per_device, mesh=mesh, in_specs=in_specs, out_specs=out_specs, check_vma=False)
```

```python
import jax
import jax.numpy as jnp
from jax import lax
from jax.experimental import pallas as pl
from jax.experimental.pallas import tpu as pltpu
from jax.sharding import PartitionSpec as P


BAND = 64
SWEEPS = 32
LANES = 128


def dot(a, b, contract=((1,), (0,))):
    return lax.dot_general(
        a, b, (contract, ((), ())), precision=lax.Precision.HIGHEST, preferred_element_type=jnp.float32
    )


def lane_of(shape):
    return lax.broadcasted_iota(jnp.int32, shape, len(shape) - 1)


def row_of(shape):
    return lax.broadcasted_iota(jnp.int32, shape, 0)


def call(kernel, outs, *args, where=None, flops=1_000_000):
    def body(*refs):
        if where is None:
            kernel(*refs)
        else:
            pl.when(where())(lambda: kernel(*refs))

    nbytes = 4 * sum(a.size for a in args)
    return pl.pallas_call(
        body,
        out_shape=[jax.ShapeDtypeStruct(s, jnp.float32) if isinstance(s, tuple) else s for s in outs],
        in_specs=[pl.BlockSpec(memory_space=pltpu.VMEM)] * len(args),
        out_specs=[pl.BlockSpec(memory_space=pltpu.VMEM)] * len(outs),
        compiler_params=pltpu.CompilerParams(vmem_limit_bytes=16 * 1024 * 1024),
        cost_estimate=pl.CostEstimate(flops=flops, bytes_accessed=nbytes, transcendentals=0),
    )(*args)


def chip_of():
    return lax.axis_index("rows") // 2


def is_north():
    return lax.axis_index("rows") % 2 == 1


def is_inside():
    index = lax.axis_index("rows")
    place = (index // 2) % 4
    return (index % 2 == 1) & ((place == 1) | (place == 2))


def split(a):
    high = a.astype(jnp.bfloat16)
    return high, (a - high.astype(jnp.float32)).astype(jnp.bfloat16)


def dot3(a, b, contract=((1,), (0,))):
    (ah, al), (bh, bl) = split(a), b if isinstance(b, tuple) else split(b)

    def one(x, y):
        return lax.dot_general(x, y, (contract, ((), ())), preferred_element_type=jnp.float32)

    return one(ah, bh) + (one(ah, bl) + one(al, bh))


def ready_kernel(x_ref, start_ref, high_ref, low_ref, column_ref):
    high_ref[...], low_ref[...] = split(x_ref[...])
    square = (SWEEPS, SWEEPS)
    row = start_ref[...].astype(jnp.float32)
    column = jnp.sum(jnp.where(lane_of(square) == row_of(square), row, 0.0), axis=1, keepdims=True)
    column_ref[...] = jnp.broadcast_to(column, (SWEEPS, LANES))


def factor_kernel(own_ref, other_ref, start_ref, high_ref, low_ref, msg_ref, inner_ref, edge_ref, solved_ref):
    first = lax.axis_index("cols") == 0
    own, other = own_ref[...], other_ref[...]
    r = jnp.concatenate([jnp.where(first, own, other), jnp.where(first, other, own)], axis=0)
    rows = r.shape[1]
    start = start_ref[:, 0:1].astype(jnp.int32)
    segment = (lane_of(r.shape) - start + BAND) >> 6
    parts = [jnp.where(segment == k, r, 0.0) for k in range(5)]
    zero = jnp.zeros_like(r)
    inner = jnp.concatenate(parts[1:4], axis=0)
    edge = jnp.concatenate([parts[0], parts[4]], axis=0)
    left = jnp.concatenate([inner, zero, edge], axis=0)
    right = jnp.concatenate([inner, zero, edge, zero, zero], axis=0)
    gram = dot3(left, right, ((1,), (1,)))
    earlier = (lane_of(gram.shape) & (SWEEPS - 1)) < (row_of(gram.shape) & (SWEEPS - 1))
    gram = jnp.where(earlier, gram, 0.0)
    count = 3 * SWEEPS
    tau = 2.0 / jnp.sum(inner * inner, axis=1, keepdims=True)
    lower = tau * gram[0:count, 0:LANES]
    rhs = tau * jnp.concatenate([inner, gram[0:count, LANES : 2 * LANES]], axis=1)
    blocks = [[rhs[32 * k + 8 * q : 32 * k + 8 * q + 8] for q in range(4)] for k in range(3)]
    for j in range(SWEEPS - 1):
        source = [blocks[k][j // 8][j % 8 : j % 8 + 1] for k in range(3)]
        for k in range(3):
            for q in range((j + 1) // 8, 4):
                at = 32 * k + 8 * q
                total = blocks[k][q]
                for m in range(3):
                    if abs(m - k) < 2:
                        column = 32 * m + j
                        total = total - lower[at : at + 8, column : column + 1] * source[m]
                blocks[k][q] = total
    solved = jnp.concatenate([blocks[k][q] for k in range(3) for q in range(4)] + [jnp.zeros((32, rhs.shape[1]), jnp.float32)], axis=0)
    back = dot3(gram[LANES : LANES + 64, 0:LANES], solved)
    observe = edge - back[:, 0:rows]
    couple = back[:, rows:] - gram[LANES : LANES + 64, LANES : 2 * LANES]
    squares = jnp.sum(edge * edge, axis=1, keepdims=True)
    coef = jnp.where(lane_of(couple.shape) == 64, squares, couple)
    inner_ref[...] = inner
    edge_ref[...] = edge
    solved_ref[...] = solved[0:count]
    upper, lower = split(observe)
    both = jnp.dot(jnp.concatenate([upper, lower], axis=0), high_ref[...], preferred_element_type=jnp.float32)
    rest = jnp.dot(upper, low_ref[...], preferred_element_type=jnp.float32)
    msg_ref[...] = jnp.concatenate([both[0:64] + (both[64:128] + rest), coef], axis=1)


def to_low(tile):
    return jnp.where(lane_of(tile.shape) < 32, pltpu.roll(tile, LANES - 32, 1), 0.0)


def solve(blocks, lower, lane=0, sweeps=SWEEPS):
    for j in range(sweeps):
        source = blocks[j // 8][j % 8 : j % 8 + 1]
        for q in range((j + 1) // 8, len(blocks)):
            blocks[q] = blocks[q] + lower[8 * q : 8 * q + 8, lane + j : lane + j + 1] * source
    return jnp.concatenate(blocks, axis=0)


def spread(rows, tile, at, solved, lane, first=0, reach=1, base=0):
    blocks = [rows[8 * q : 8 * q + 8] for q in range(rows.shape[0] // 8)]
    for j in range(solved.shape[0]):
        for q in range(len(blocks)):
            top = at + 8 * q
            if top + 7 >= first + j + reach:
                column = lane + first + j
                blocks[q] = blocks[q] + tile[top - base : top - base + 8, column : column + 1] * solved[j : j + 1]
    return blocks[0] if len(blocks) == 1 else jnp.concatenate(blocks, axis=0)


def substitute(block, lower, first, lane):
    for j in range(block.shape[0] - 1):
        block = block + lower[first : first + block.shape[0], lane + first + j : lane + first + j + 1] * block[j : j + 1]
    return block


def merge_kernel(own_ref, got_ref, mid_ref, first_ref, rest_ref):
    even = chip_of() % 2 == 0
    cols = own_ref.shape[1] - LANES
    top, low = got_ref[...], own_ref[...]
    tc, lc = top[:, cols:], low[:, cols:]
    tau = 2.0 / (tc[32:64, 64:65] + lc[0:32, 64:65])
    lane = lane_of(tc.shape)
    tk = jnp.where(lane < 32, tc, 0.0)
    lk = jnp.where((lane >= 32) & (lane < 64), lc, 0.0)
    mid = jnp.concatenate([top[32:64, 0:cols] + low[0:32, 0:cols], tk[32:64] + lk[0:32]], axis=1) * tau
    left = jnp.concatenate([top[0:32, 0:cols], tk[0:32]], axis=1)
    right = jnp.concatenate([low[32:64, 0:cols], lk[32:64]], axis=1)
    weights = (pltpu.roll(tc[32:64], LANES - 32, 1) + lc[0:32]) * tau
    mid = solve([mid[8 * q : 8 * q + 8] for q in range(4)], weights)
    left = spread(left, tc[0:32], 0, mid, 32, reach=4)
    right = spread(right, lc[32:64], 0, mid, 0, reach=4)

    def ordered(block):
        tile = block[:, cols:]
        at = lane_of(tile.shape)
        swapped = jnp.where(at < 32, pltpu.roll(tile, 96, 1), pltpu.roll(tile, 32, 1))
        return jnp.where(at < 64, jnp.where(even, swapped, tile), 0.0)

    spot = lane_of((32, LANES)) == 64
    left = jnp.concatenate([left[:, 0:cols], jnp.where(spot, tc[0:32, 64:65], ordered(left))], axis=1)
    right = jnp.concatenate([right[:, 0:cols], jnp.where(spot, lc[32:64, 64:65], ordered(right))], axis=1)
    mid_ref[...] = jnp.concatenate([mid[:, 0:cols], ordered(mid)], axis=1)
    e = jnp.where(even, right, left)
    first_ref[...] = e[0:8]
    rest_ref[...] = jnp.concatenate([e[8:32], jnp.where(even, left, right)], axis=0)


def pair_kernel(first_ref, rest_ref, got_ref, msg_ref):
    cols = first_ref.shape[1] - LANES
    both = first_ref[...] + got_ref[...]
    tau = 2.0 / both[:, cols + 64 : cols + 65]
    e = substitute(both[:, 0:cols] * tau, tau * both[:, cols:], 0, 0)
    tile = rest_ref[24:56, cols:]
    p = spread(rest_ref[24:40, 0:cols], tile, 0, e, 0, reach=8)
    msg_ref[...] = jnp.concatenate([p, tile[0:16], tile[16:32]], axis=1)


def joined(own, got):
    cols = own.shape[1] - LANES
    mine, theirs = own[:, cols:], got[:, cols:]
    tau = 2.0 / (mine[:, 64:65] + theirs[:, 64:65])
    lane = lane_of(mine.shape)
    outer = to_low(theirs) + jnp.where((lane >= 32) & (lane < 64), mine, 0.0)
    return jnp.concatenate([own[:, 0:cols] + got[:, 0:cols], outer], axis=1) * tau, tau * (mine + theirs)


def edges_kernel(first_ref, rest_ref, got_first_ref, got_rest_ref, pair_ref, w_ref):
    cols = first_ref.shape[1] - LANES
    pair, lower = joined(
        jnp.concatenate([first_ref[...], rest_ref[0:16]], axis=0),
        jnp.concatenate([got_first_ref[...], got_rest_ref[0:16]], axis=0),
    )
    pair = solve([pair[8 * q : 8 * q + 8] for q in range(3)], lower, sweeps=24)
    pair_ref[...] = pair
    tile = got_rest_ref[24:56, cols:]
    kept = to_low(tile) + jnp.where(lane_of(tile.shape) == 64, tile, 0.0)
    w = jnp.concatenate([got_rest_ref[24:56, 0:cols], kept], axis=1)
    w_ref[...] = spread(w, tile, 0, pair, 0, reach=8)


def late_kernel(rest_ref, got_rest_ref, pair_ref, last_ref, p_ref):
    cols = rest_ref.shape[1] - LANES
    pair = pair_ref[...]
    last, lower = joined(rest_ref[16:24], got_rest_ref[16:24])
    last = spread(last, lower, 24, pair, 0, base=24)
    for j in range(7):
        last = last + lower[:, 24 + j : 25 + j] * last[j : j + 1]
    last_ref[...] = last
    tile = rest_ref[40:56, cols:]
    lane = lane_of(tile.shape)
    p = jnp.concatenate([rest_ref[40:56, 0:cols], jnp.where((lane >= 32) & (lane < 64), tile, 0.0)], axis=1)
    p_ref[...] = spread(p, tile, 16, pair, 0, reach=8, base=16)


def p0_kernel(msg_ref, own_ref, w_ref, p0_ref, scaled_ref, out_ref):
    cols = w_ref.shape[1] - LANES
    both = own_ref[...] + msg_ref[...]
    tile = jnp.concatenate([both[:, cols : cols + LANES], both[:, cols + LANES :]], axis=0)
    tau = 2.0 / tile[:, 64:65]
    lower = tau * tile
    scaled_ref[...] = jnp.where(lane_of(lower.shape) == 64, tau, lower)
    p0 = substitute(both[:, 0:cols] * tau[0:16], lower, 0, 32)
    p0_ref[...] = p0
    tile = w_ref[:, cols:]
    w = jnp.concatenate([w_ref[0:16, 0:cols], spread(w_ref[16:32, 0:cols], tile, 16, p0, 32, reach=16)], axis=0)
    out_ref[...] = jnp.concatenate([w, tile], axis=1)


def w_kernel(msg_ref, start_ref, w_ref, p_ref, p0_ref, out_w_ref, out_ref):
    cols = w_ref.shape[1] - LANES
    chip = chip_of()
    chips = lax.axis_size("rows") // 2
    start = start_ref[:, 0:1]
    valid = (chip != 1) & ((chip != chips - 2) | (start == 0.0))
    got = jnp.where((chip != 1) & (chip != chips - 2), msg_ref[...], 0.0)
    both = w_ref[...] + got
    squares = both[:, cols + 64 : cols + 65]
    tau = jnp.where(valid, 2.0 / jnp.where(valid, squares, 1.0), 0.0)
    w = both[:, 0:cols] * tau
    w = solve([w[8 * q : 8 * q + 8] for q in range(4)], tau * both[:, cols:])
    out_w_ref[...] = w
    tile = p_ref[:, cols:]
    rest = spread(p_ref[:, 0:cols], tile, 16, p0_ref[...], 32, base=16)
    out_ref[...] = spread(rest, tile, 16, w[0:16], 0, reach=16, base=16)


def e0_kernel(pair_ref, last_ref, w_ref, p0_ref, out_ref, tail_ref):
    cols = w_ref.shape[1]
    w, p0 = w_ref[0:24], p0_ref[...]
    e = spread(pair_ref[:, 0:cols], pair_ref[:, cols:], 0, w[0:16], 0, reach=8)
    out_ref[...] = jnp.concatenate([w_ref[...], spread(e, pair_ref[:, cols:], 0, p0, 32, reach=8)], axis=0)
    tail = spread(last_ref[:, 0:cols], last_ref[:, cols:], 24, w, 0, reach=8, base=24)
    tail_ref[...] = spread(tail, last_ref[:, cols:], 24, p0, 32, reach=8, base=24)


def p1_kernel(msg_ref, scaled_ref, rest_ref, last_ref, tail_ref, p0_ref, p_ref, out_ref):
    cols = msg_ref.shape[1]
    scaled = scaled_ref[...]
    p1 = substitute((rest_ref[...] + msg_ref[...]) * scaled[16:32, 64:65], scaled, 16, 32)
    p_ref[...] = jnp.concatenate([p0_ref[...], p1], axis=0)
    out_ref[...] = spread(tail_ref[...], last_ref[:, cols:], 24, p1[0:8], 32, first=16, reach=8, base=24)


def mid_kernel(mid_ref, p_ref, own_ref, got_ref, part_ref, o_ref, e_ref):
    cols = p_ref.shape[1]
    inside = is_inside()
    o = jnp.where(inside, p_ref[...], got_ref[0:32])
    e = jnp.where(inside, own_ref[32:56], got_ref[32:56])
    tile = mid_ref[:, cols:]
    o_ref[...] = o
    e_ref[...] = e
    part_ref[...] = spread(spread(mid_ref[:, 0:cols], tile, 0, e, 0, reach=4), tile, 0, o, 32, reach=4)


def back_kernel(mid_ref, part_ref, o_ref, e_ref, own_ref, got_ref, keep_ref, out_ref):
    cols = o_ref.shape[1]
    even = chip_of() % 2 == 0
    tail = jnp.where(is_inside(), own_ref[...], got_ref[...])
    last = spread(part_ref[24:32], mid_ref[:, cols:], 24, tail, 0, first=24, reach=4)
    for q in range(4):
        at = slice(8 * q, 8 * q + 8)
        below = slice(32 + 8 * q, 40 + 8 * q)
        e = tail if q == 3 else e_ref[at]
        mid = last if q == 3 else part_ref[at]
        o = o_ref[at]
        out_ref[at] = jnp.where(even, o, e)
        out_ref[below] = mid
        keep_ref[at] = mid
        keep_ref[below] = jnp.where(even, e, o)


def inner_kernel(inner_ref, edge_ref, solved_ref, high_ref, low_ref, x_ref, y_ref, lhs_ref):
    rows = x_ref.shape[0]
    inner = inner_ref[...]
    part = dot3(solved_ref[:, 0:rows], (high_ref[...], low_ref[...]))
    y_ref[...] = x_ref[...] - dot3(inner, part, ((0,), (0,)))
    edge = edge_ref[...] - dot(solved_ref[:, rows : rows + 64], inner, ((0,), (0,)))
    high = edge.astype(jnp.bfloat16).astype(jnp.float32)
    stack = jnp.concatenate([high, high, edge - high, jnp.zeros_like(edge)], axis=0)
    lhs_ref[...] = stack.T.astype(jnp.bfloat16)


def final_kernel(lhs_ref, keep_ref, msg_ref, y_ref, out_ref, piece_ref, sems):
    north = is_north()
    lhs = lhs_ref[...]
    width = piece_ref.shape[2]
    copies = []
    for i in range(piece_ref.shape[0]):
        at = slice(i * width, (i + 1) * width)
        high, low = split(jnp.where(north, keep_ref[:, at], msg_ref[:, at]))
        rhs = jnp.concatenate([high, low, high, jnp.zeros_like(high)], axis=0)
        piece_ref[i] = y_ref[:, at] - jnp.dot(lhs, rhs, preferred_element_type=jnp.float32)
        copy = pltpu.make_async_copy(piece_ref.at[i], out_ref.at[:, at], sems.at[i])
        copy.start()
        copies.append(copy)
    for copy in copies:
        copy.wait()


def trade(array, pairs):
    return lax.ppermute(array, "rows", pairs)


def per_device(eigvecs, reflectors, starts):
    count = lax.axis_size("rows")
    chips = count // 2
    rows, cols = eigvecs.shape
    wide = cols + LANES

    far = 32 if count >= 64 else 8

    def swap(pick):
        return [(i, pick(i, i // 2, i % 2 == 1, (i // 2) % 4 in (1, 2))) for i in range(count)]

    def next_quad(i, chip, north, inside):
        end = chip < 2 or chip >= chips - 2
        if end and not inside:
            return None if north else i + 3 if chip == 0 else i - 1
        if north and inside:
            return i - 3 if chip == 1 else i + 1 if end else i + 6 if chip % 4 == 2 else i - 6
        return i ^ far if inside else i ^ 1

    on_chip = swap(lambda i, chip, north, inside: i ^ 1)
    in_pair = swap(lambda i, chip, north, inside: i ^ 2 if north else i ^ 8)
    p_pairs = swap(lambda i, chip, north, inside: (i ^ 6 if north else i ^ far) if inside else i ^ 1)
    w_pairs = [
        (2 * i + c, 2 * i + 1 - c if j is None else 2 * j + c) for i, j in swap(next_quad) for c in range(2)
    ]
    other = lax.ppermute(reflectors, "cols", [(0, 1), (1, 0)])
    half = jax.ShapeDtypeStruct(eigvecs.shape, jnp.bfloat16)
    high, low, start = call(ready_kernel, [half, half, (SWEEPS, LANES)], eigvecs, starts[None, :], flops=20_000_000)
    msg, inner, edge, solved = call(
        factor_kernel, [(64, wide), (96, rows), (64, rows), (96, rows + LANES)], reflectors, other, start, high, low
    )
    got = lax.ppermute(msg, "rows", on_chip)
    mid, first, rest = call(merge_kernel, [(32, wide), (8, wide), (56, wide)], msg, got, where=is_north)
    got_first = trade(first, in_pair)
    got_rest = trade(rest, in_pair)
    (msg,) = call(pair_kernel, [(16, wide + LANES)], first, rest, got_first, where=is_inside)
    got = trade(msg, p_pairs)
    pair, w = call(edges_kernel, [(24, wide), (32, wide)], first, rest, got_first, got_rest, where=is_inside)
    p0, scaled, w = call(p0_kernel, [(16, cols), (32, LANES), (32, wide)], got, msg, w, where=is_inside)
    got = lax.ppermute(w, ("rows", "cols"), w_pairs)
    last, p = call(late_kernel, [(8, wide), (16, wide)], rest, got_rest, pair, where=is_inside)
    partial, lhs = call(
        inner_kernel, [(rows, cols), jax.ShapeDtypeStruct((rows, 256), jnp.bfloat16)],
        inner, edge, solved, high, low, eigvecs, flops=20_000_000,
    )
    w, rest = call(w_kernel, [(32, cols), (16, cols)], got, start, w, p, p0, where=is_inside)
    most, tail = call(e0_kernel, [(56, cols), (8, cols)], pair, last, w, p0, where=is_inside)
    got_most = trade(most, in_pair)
    got = trade(rest, p_pairs)
    p, tail = call(p1_kernel, [(32, cols), (8, cols)], got, scaled, rest, last, tail, p0, where=is_inside)
    got = lax.ppermute(tail, "rows", in_pair)
    part, o, e = call(mid_kernel, [(32, cols), (32, cols), (24, cols)], mid, p, most, got_most, where=is_north)
    keep, msg = call(back_kernel, [(64, cols), (64, cols)], mid, part, o, e, tail, got, where=is_north)
    got = lax.ppermute(msg, "rows", on_chip)
    return pl.pallas_call(
        final_kernel,
        out_shape=jax.ShapeDtypeStruct((rows, cols), jnp.float32),
        in_specs=[pl.BlockSpec(memory_space=pltpu.VMEM)] * 4,
        out_specs=pl.BlockSpec(memory_space=pl.ANY),
        scratch_shapes=[pltpu.VMEM((4, rows, cols // 4), jnp.float32), pltpu.SemaphoreType.DMA((4,))],
        compiler_params=pltpu.CompilerParams(vmem_limit_bytes=16 * 1024 * 1024),
    )(lhs, keep, got, partial)


def solution(mesh):
    in_specs = (P("rows", "cols"), P("cols", "rows"), P())
    out_specs = P("rows", "cols")

    return jax.shard_map(per_device, mesh=mesh, in_specs=in_specs, out_specs=out_specs, check_vma=False)
```

```python
import jax
import jax.numpy as jnp
from jax import lax
from jax.experimental import pallas as pl
from jax.experimental.pallas import tpu as pltpu
from jax.sharding import PartitionSpec as P


BAND = 64
SWEEPS = 32
LANES = 128


def dot(a, b, contract=((1,), (0,))):
    return lax.dot_general(
        a, b, (contract, ((), ())), precision=lax.Precision.HIGHEST, preferred_element_type=jnp.float32
    )


def lane_of(shape):
    return lax.broadcasted_iota(jnp.int32, shape, len(shape) - 1)


def row_of(shape):
    return lax.broadcasted_iota(jnp.int32, shape, 0)


def call(kernel, outs, *args, where=None, flops=1_000_000):
    def body(*refs):
        if where is None:
            kernel(*refs)
        else:
            pl.when(where())(lambda: kernel(*refs))

    nbytes = 4 * sum(a.size for a in args)
    return pl.pallas_call(
        body,
        out_shape=[jax.ShapeDtypeStruct(s, jnp.float32) if isinstance(s, tuple) else s for s in outs],
        in_specs=[pl.BlockSpec(memory_space=pltpu.VMEM)] * len(args),
        out_specs=[pl.BlockSpec(memory_space=pltpu.VMEM)] * len(outs),
        compiler_params=pltpu.CompilerParams(vmem_limit_bytes=16 * 1024 * 1024),
        cost_estimate=pl.CostEstimate(flops=flops, bytes_accessed=nbytes, transcendentals=0),
    )(*args)


def chip_of():
    return lax.axis_index("rows") // 2


def is_north():
    return lax.axis_index("rows") % 2 == 1


def is_inside():
    index = lax.axis_index("rows")
    place = (index // 2) % 4
    return (index % 2 == 1) & ((place == 1) | (place == 2))


def split(a):
    high = a.astype(jnp.bfloat16)
    return high, (a - high.astype(jnp.float32)).astype(jnp.bfloat16)


def dot3(a, b, contract=((1,), (0,))):
    (ah, al), (bh, bl) = split(a), b if isinstance(b, tuple) else split(b)

    def one(x, y):
        return lax.dot_general(x, y, (contract, ((), ())), preferred_element_type=jnp.float32)

    return one(ah, bh) + (one(ah, bl) + one(al, bh))


def ready_kernel(start_ref, column_ref):
    square = (SWEEPS, SWEEPS)
    row = start_ref[...].astype(jnp.float32)
    column = jnp.sum(jnp.where(lane_of(square) == row_of(square), row, 0.0), axis=1, keepdims=True)
    column_ref[...] = jnp.broadcast_to(column, (SWEEPS, LANES))


def factor_kernel(own_ref, other_ref, start_ref, observe_ref, coef_ref, inner_ref, edge_ref, solved_ref):
    first = lax.axis_index("cols") == 0
    own, other = own_ref[...], other_ref[...]
    r = jnp.concatenate([jnp.where(first, own, other), jnp.where(first, other, own)], axis=0)
    rows = r.shape[1]
    start = start_ref[:, 0:1].astype(jnp.int32)
    segment = (lane_of(r.shape) - start + BAND) >> 6
    parts = [jnp.where(segment == k, r, 0.0) for k in range(5)]
    zero = jnp.zeros_like(r)
    inner = jnp.concatenate(parts[1:4], axis=0)
    edge = jnp.concatenate([parts[0], parts[4]], axis=0)
    left = jnp.concatenate([inner, edge], axis=0)
    right = jnp.concatenate([inner, zero, edge, zero, zero], axis=0)
    gram = dot3(left, right, ((1,), (1,)))
    earlier = (lane_of(gram.shape) & (SWEEPS - 1)) < (row_of(gram.shape) & (SWEEPS - 1))
    gram = jnp.where(earlier, gram, 0.0)
    count = 3 * SWEEPS
    tau = 2.0 / jnp.sum(inner * inner, axis=1, keepdims=True)
    lower = tau * gram[0:count, 0:LANES]
    rhs = tau * jnp.concatenate([inner, gram[0:count, LANES : 2 * LANES]], axis=1)
    blocks = [[rhs[32 * k + 8 * q : 32 * k + 8 * q + 8] for q in range(4)] for k in range(3)]
    for j in range(SWEEPS - 1):
        source = [blocks[k][j // 8][j % 8 : j % 8 + 1] for k in range(3)]
        for k in range(3):
            for q in range((j + 1) // 8, 4):
                at = 32 * k + 8 * q
                total = blocks[k][q]
                for m in range(3):
                    if abs(m - k) < 2:
                        column = 32 * m + j
                        total = total - lower[at : at + 8, column : column + 1] * source[m]
                blocks[k][q] = total
    solved = jnp.concatenate([blocks[k][q] for k in range(3) for q in range(4)] + [jnp.zeros((32, rhs.shape[1]), jnp.float32)], axis=0)
    back = dot3(gram[count : count + 64, 0:LANES], solved)
    observe = edge - back[:, 0:rows]
    couple = back[:, rows:] - gram[count : count + 64, LANES : 2 * LANES]
    squares = jnp.sum(edge * edge, axis=1, keepdims=True)
    coef = jnp.where(lane_of(couple.shape) == 64, squares, couple)
    inner_ref[...] = inner
    edge_ref[...] = edge
    solved_ref[...] = solved[0:count]
    observe_ref[...] = observe
    coef_ref[...] = coef


def project_kernel(observe_ref, coef_ref, x_ref, msg_ref):
    upper, lower = split(observe_ref[...])
    high, low = split(x_ref[...])
    both = jnp.dot(jnp.concatenate([upper, lower], axis=0), high, preferred_element_type=jnp.float32)
    rest = jnp.dot(upper, low, preferred_element_type=jnp.float32)
    msg_ref[...] = jnp.concatenate([both[0:64] + (both[64:128] + rest), coef_ref[...]], axis=1)


def to_low(tile):
    return jnp.where(lane_of(tile.shape) < 32, pltpu.roll(tile, LANES - 32, 1), 0.0)


def solve(blocks, lower, lane=0, sweeps=SWEEPS):
    for j in range(sweeps):
        source = blocks[j // 8][j % 8 : j % 8 + 1]
        for q in range((j + 1) // 8, len(blocks)):
            blocks[q] = blocks[q] + lower[8 * q : 8 * q + 8, lane + j : lane + j + 1] * source
    return jnp.concatenate(blocks, axis=0)


def spread(rows, tile, at, solved, lane, first=0, reach=1, base=0):
    blocks = [rows[8 * q : 8 * q + 8] for q in range(rows.shape[0] // 8)]
    for j in range(solved.shape[0]):
        for q in range(len(blocks)):
            top = at + 8 * q
            if top + 7 >= first + j + reach:
                column = lane + first + j
                blocks[q] = blocks[q] + tile[top - base : top - base + 8, column : column + 1] * solved[j : j + 1]
    return blocks[0] if len(blocks) == 1 else jnp.concatenate(blocks, axis=0)


def substitute(block, lower, first, lane):
    for j in range(block.shape[0] - 1):
        block = block + lower[first : first + block.shape[0], lane + first + j : lane + first + j + 1] * block[j : j + 1]
    return block


def merge_kernel(own_ref, got_ref, mid_ref, first_ref, rest_ref):
    even = chip_of() % 2 == 0
    cols = own_ref.shape[1] - LANES
    top, low = got_ref[...], own_ref[...]
    tc, lc = top[:, cols:], low[:, cols:]
    tau = 2.0 / (tc[32:64, 64:65] + lc[0:32, 64:65])
    lane = lane_of(tc.shape)
    tk = jnp.where(lane < 32, tc, 0.0)
    lk = jnp.where((lane >= 32) & (lane < 64), lc, 0.0)
    mid = jnp.concatenate([top[32:64, 0:cols] + low[0:32, 0:cols], tk[32:64] + lk[0:32]], axis=1) * tau
    left = jnp.concatenate([top[0:32, 0:cols], tk[0:32]], axis=1)
    right = jnp.concatenate([low[32:64, 0:cols], lk[32:64]], axis=1)
    weights = (pltpu.roll(tc[32:64], LANES - 32, 1) + lc[0:32]) * tau
    mid = solve([mid[8 * q : 8 * q + 8] for q in range(4)], weights)
    left = spread(left, tc[0:32], 0, mid, 32, reach=4)
    right = spread(right, lc[32:64], 0, mid, 0, reach=4)

    def ordered(block):
        tile = block[:, cols:]
        at = lane_of(tile.shape)
        swapped = jnp.where(at < 32, pltpu.roll(tile, 96, 1), pltpu.roll(tile, 32, 1))
        return jnp.where(at < 64, jnp.where(even, swapped, tile), 0.0)

    spot = lane_of((32, LANES)) == 64
    left = jnp.concatenate([left[:, 0:cols], jnp.where(spot, tc[0:32, 64:65], ordered(left))], axis=1)
    right = jnp.concatenate([right[:, 0:cols], jnp.where(spot, lc[32:64, 64:65], ordered(right))], axis=1)
    mid_ref[...] = jnp.concatenate([mid[:, 0:cols], ordered(mid)], axis=1)
    e = jnp.where(even, right, left)
    first_ref[...] = e[0:8]
    rest_ref[...] = jnp.concatenate([e[8:32], jnp.where(even, left, right)], axis=0)


def pair_kernel(first_ref, rest_ref, got_ref, msg_ref):
    cols = first_ref.shape[1] - LANES
    both = first_ref[...] + got_ref[...]
    tau = 2.0 / both[:, cols + 64 : cols + 65]
    e = substitute(both[:, 0:cols] * tau, tau * both[:, cols:], 0, 0)
    tile = rest_ref[24:56, cols:]
    p = spread(rest_ref[24:40, 0:cols], tile, 0, e, 0, reach=8)
    msg_ref[...] = jnp.concatenate([p, tile[0:16], tile[16:32]], axis=1)


def joined(own, got):
    cols = own.shape[1] - LANES
    mine, theirs = own[:, cols:], got[:, cols:]
    tau = 2.0 / (mine[:, 64:65] + theirs[:, 64:65])
    lane = lane_of(mine.shape)
    outer = to_low(theirs) + jnp.where((lane >= 32) & (lane < 64), mine, 0.0)
    return jnp.concatenate([own[:, 0:cols] + got[:, 0:cols], outer], axis=1) * tau, tau * (mine + theirs)


def edges_kernel(first_ref, rest_ref, got_first_ref, got_rest_ref, pair_ref, w_ref):
    cols = first_ref.shape[1] - LANES
    pair, lower = joined(
        jnp.concatenate([first_ref[...], rest_ref[0:16]], axis=0),
        jnp.concatenate([got_first_ref[...], got_rest_ref[0:16]], axis=0),
    )
    pair = solve([pair[8 * q : 8 * q + 8] for q in range(3)], lower, sweeps=24)
    pair_ref[...] = pair
    tile = got_rest_ref[24:56, cols:]
    kept = to_low(tile) + jnp.where(lane_of(tile.shape) == 64, tile, 0.0)
    w = jnp.concatenate([got_rest_ref[24:56, 0:cols], kept], axis=1)
    w_ref[...] = spread(w, tile, 0, pair, 0, reach=8)


def late_kernel(rest_ref, got_rest_ref, pair_ref, last_ref, p_ref):
    cols = rest_ref.shape[1] - LANES
    pair = pair_ref[...]
    last, lower = joined(rest_ref[16:24], got_rest_ref[16:24])
    last = spread(last, lower, 24, pair, 0, base=24)
    for j in range(7):
        last = last + lower[:, 24 + j : 25 + j] * last[j : j + 1]
    last_ref[...] = last
    tile = rest_ref[40:56, cols:]
    lane = lane_of(tile.shape)
    p = jnp.concatenate([rest_ref[40:56, 0:cols], jnp.where((lane >= 32) & (lane < 64), tile, 0.0)], axis=1)
    p_ref[...] = spread(p, tile, 16, pair, 0, reach=8, base=16)


def p0_kernel(msg_ref, own_ref, w_ref, p0_ref, scaled_ref, out_ref):
    cols = w_ref.shape[1] - LANES
    both = own_ref[...] + msg_ref[...]
    tile = jnp.concatenate([both[:, cols : cols + LANES], both[:, cols + LANES :]], axis=0)
    tau = 2.0 / tile[:, 64:65]
    lower = tau * tile
    scaled_ref[...] = jnp.where(lane_of(lower.shape) == 64, tau, lower)
    p0 = substitute(both[:, 0:cols] * tau[0:16], lower, 0, 32)
    p0_ref[...] = p0
    tile = w_ref[:, cols:]
    w = jnp.concatenate([w_ref[0:16, 0:cols], spread(w_ref[16:32, 0:cols], tile, 16, p0, 32, reach=16)], axis=0)
    out_ref[...] = jnp.concatenate([w, tile], axis=1)


def w_kernel(msg_ref, start_ref, w_ref, p_ref, p0_ref, out_w_ref, out_ref):
    cols = w_ref.shape[1] - LANES
    chip = chip_of()
    chips = lax.axis_size("rows") // 2
    start = start_ref[:, 0:1]
    valid = (chip != 1) & ((chip != chips - 2) | (start == 0.0))
    got = jnp.where((chip != 1) & (chip != chips - 2), msg_ref[...], 0.0)
    both = w_ref[...] + got
    squares = both[:, cols + 64 : cols + 65]
    tau = jnp.where(valid, 2.0 / jnp.where(valid, squares, 1.0), 0.0)
    w = both[:, 0:cols] * tau
    w = solve([w[8 * q : 8 * q + 8] for q in range(4)], tau * both[:, cols:])
    out_w_ref[...] = w
    tile = p_ref[:, cols:]
    rest = spread(p_ref[:, 0:cols], tile, 16, p0_ref[...], 32, base=16)
    out_ref[...] = spread(rest, tile, 16, w[0:16], 0, reach=16, base=16)


def e0_kernel(pair_ref, last_ref, w_ref, p0_ref, out_ref, tail_ref):
    cols = w_ref.shape[1]
    w, p0 = w_ref[0:24], p0_ref[...]
    e = spread(pair_ref[:, 0:cols], pair_ref[:, cols:], 0, w[0:16], 0, reach=8)
    out_ref[...] = jnp.concatenate([w_ref[...], spread(e, pair_ref[:, cols:], 0, p0, 32, reach=8)], axis=0)
    tail = spread(last_ref[:, 0:cols], last_ref[:, cols:], 24, w, 0, reach=8, base=24)
    tail_ref[...] = spread(tail, last_ref[:, cols:], 24, p0, 32, reach=8, base=24)


def p1_kernel(msg_ref, scaled_ref, rest_ref, last_ref, tail_ref, p0_ref, p_ref, out_ref):
    cols = msg_ref.shape[1]
    scaled = scaled_ref[...]
    p1 = substitute((rest_ref[...] + msg_ref[...]) * scaled[16:32, 64:65], scaled, 16, 32)
    p_ref[...] = jnp.concatenate([p0_ref[...], p1], axis=0)
    out_ref[...] = spread(tail_ref[...], last_ref[:, cols:], 24, p1[0:8], 32, first=16, reach=8, base=24)


def mid_kernel(mid_ref, p_ref, own_ref, got_ref, part_ref, o_ref, e_ref):
    cols = p_ref.shape[1]
    inside = is_inside()
    o = jnp.where(inside, p_ref[...], got_ref[0:32])
    e = jnp.where(inside, own_ref[32:56], got_ref[32:56])
    tile = mid_ref[:, cols:]
    o_ref[...] = o
    e_ref[...] = e
    part_ref[...] = spread(spread(mid_ref[:, 0:cols], tile, 0, e, 0, reach=4), tile, 0, o, 32, reach=4)


def back_kernel(mid_ref, part_ref, o_ref, e_ref, own_ref, got_ref, keep_ref, out_ref):
    cols = o_ref.shape[1]
    even = chip_of() % 2 == 0
    tail = jnp.where(is_inside(), own_ref[...], got_ref[...])
    last = spread(part_ref[24:32], mid_ref[:, cols:], 24, tail, 0, first=24, reach=4)
    for q in range(4):
        at = slice(8 * q, 8 * q + 8)
        below = slice(32 + 8 * q, 40 + 8 * q)
        e = tail if q == 3 else e_ref[at]
        mid = last if q == 3 else part_ref[at]
        o = o_ref[at]
        out_ref[at] = jnp.where(even, o, e)
        out_ref[below] = mid
        keep_ref[at] = mid
        keep_ref[below] = jnp.where(even, e, o)


def inner_kernel(inner_ref, edge_ref, solved_ref, x_ref, y_ref, lhs_ref):
    rows = x_ref.shape[0]
    inner = inner_ref[...]
    part = dot3(solved_ref[:, 0:rows], x_ref[...])
    y_ref[...] = x_ref[...] - dot3(inner, part, ((0,), (0,)))
    edge = edge_ref[...] - dot(solved_ref[:, rows : rows + 64], inner, ((0,), (0,)))
    high = edge.astype(jnp.bfloat16).astype(jnp.float32)
    stack = jnp.concatenate([high, high, edge - high, jnp.zeros_like(edge)], axis=0)
    lhs_ref[...] = stack.T.astype(jnp.bfloat16)


def final_kernel(lhs_ref, keep_ref, msg_ref, y_ref, out_ref, piece_ref, sems):
    north = is_north()
    lhs = lhs_ref[...]
    width = piece_ref.shape[2]
    copies = []
    for i in range(piece_ref.shape[0]):
        at = slice(i * width, (i + 1) * width)
        high, low = split(jnp.where(north, keep_ref[:, at], msg_ref[:, at]))
        rhs = jnp.concatenate([high, low, high, jnp.zeros_like(high)], axis=0)
        piece_ref[i] = y_ref[:, at] - jnp.dot(lhs, rhs, preferred_element_type=jnp.float32)
        copy = pltpu.make_async_copy(piece_ref.at[i], out_ref.at[:, at], sems.at[i])
        copy.start()
        copies.append(copy)
    for copy in copies:
        copy.wait()


def trade(array, pairs):
    return lax.ppermute(array, "rows", pairs)


def per_device(eigvecs, reflectors, starts):
    count = lax.axis_size("rows")
    chips = count // 2
    rows, cols = eigvecs.shape
    wide = cols + LANES

    far = 32 if count >= 64 else 8

    def swap(pick):
        return [(i, pick(i, i // 2, i % 2 == 1, (i // 2) % 4 in (1, 2))) for i in range(count)]

    def next_quad(i, chip, north, inside):
        end = chip < 2 or chip >= chips - 2
        if end and not inside:
            return None if north else i + 3 if chip == 0 else i - 1
        if north and inside:
            return i - 3 if chip == 1 else i + 1 if end else i + 6 if chip % 4 == 2 else i - 6
        return i ^ far if inside else i ^ 1

    on_chip = swap(lambda i, chip, north, inside: i ^ 1)
    in_pair = swap(lambda i, chip, north, inside: i ^ 2 if north else i ^ 8)
    p_pairs = swap(lambda i, chip, north, inside: (i ^ 6 if north else i ^ far) if inside else i ^ 1)
    w_pairs = [
        (2 * i + c, 2 * i + 1 - c if j is None else 2 * j + c) for i, j in swap(next_quad) for c in range(2)
    ]
    other = lax.ppermute(reflectors, "cols", [(0, 1), (1, 0)])
    (start,) = call(ready_kernel, [(SWEEPS, LANES)], starts[None, :], flops=20_000_000)
    observe, coef, inner, edge, solved = call(
        factor_kernel,
        [(64, rows), (64, LANES), (96, rows), (64, rows), (96, rows + LANES)],
        reflectors, other, start,
        flops=2_000_000_000,
    )
    (msg,) = call(project_kernel, [(64, wide)], observe, coef, eigvecs)
    got = lax.ppermute(msg, "rows", on_chip)
    mid, first, rest = call(merge_kernel, [(32, wide), (8, wide), (56, wide)], msg, got, where=is_north)
    got_first = trade(first, in_pair)
    got_rest = trade(rest, in_pair)
    (msg,) = call(pair_kernel, [(16, wide + LANES)], first, rest, got_first, where=is_inside)
    got = trade(msg, p_pairs)
    pair, w = call(edges_kernel, [(24, wide), (32, wide)], first, rest, got_first, got_rest, where=is_inside)
    p0, scaled, w = call(p0_kernel, [(16, cols), (32, LANES), (32, wide)], got, msg, w, where=is_inside)
    got = lax.ppermute(w, ("rows", "cols"), w_pairs)
    last, p = call(late_kernel, [(8, wide), (16, wide)], rest, got_rest, pair, where=is_inside)
    partial, lhs = call(
        inner_kernel, [(rows, cols), jax.ShapeDtypeStruct((rows, 256), jnp.bfloat16)],
        inner, edge, solved, eigvecs, flops=20_000_000,
    )
    w, rest = call(w_kernel, [(32, cols), (16, cols)], got, start, w, p, p0, where=is_inside)
    most, tail = call(e0_kernel, [(56, cols), (8, cols)], pair, last, w, p0, where=is_inside)
    got_most = trade(most, in_pair)
    got = trade(rest, p_pairs)
    p, tail = call(p1_kernel, [(32, cols), (8, cols)], got, scaled, rest, last, tail, p0, where=is_inside)
    got = lax.ppermute(tail, "rows", in_pair)
    part, o, e = call(mid_kernel, [(32, cols), (32, cols), (24, cols)], mid, p, most, got_most, where=is_north)
    keep, msg = call(back_kernel, [(64, cols), (64, cols)], mid, part, o, e, tail, got, where=is_north)
    got = lax.ppermute(msg, "rows", on_chip)
    return pl.pallas_call(
        final_kernel,
        out_shape=jax.ShapeDtypeStruct((rows, cols), jnp.float32),
        in_specs=[pl.BlockSpec(memory_space=pltpu.VMEM)] * 4,
        out_specs=pl.BlockSpec(memory_space=pl.ANY),
        scratch_shapes=[pltpu.VMEM((2, rows, cols // 2), jnp.float32), pltpu.SemaphoreType.DMA((2,))],
        compiler_params=pltpu.CompilerParams(vmem_limit_bytes=16 * 1024 * 1024),
    )(lhs, keep, got, partial)


def solution(mesh):
    in_specs = (P("rows", "cols"), P("cols", "rows"), P())
    out_specs = P("rows", "cols")

    return jax.shard_map(per_device, mesh=mesh, in_specs=in_specs, out_specs=out_specs, check_vma=False)
```
